256 devices in a mesh: dp: 64 (over x, z, core), tensor: 4 (over y).
Axes of the slice: x: 4, y: 4, z: 8, core: 2. Of those that a mesh axis runs over, the one named last changes fastest.
Arguments:
- attn_out: bfloat16 [32768, 2560], P('dp', 'tensor'), may hold values from -6 to 6
- resid: bfloat16 [32768, 5120], P('dp', 'tensor'), may hold values from -6 to 6
- out_proj: bfloat16 [2560, 5120], P('tensor'), may hold values from -0.125 to 0.125
- heads: bfloat16 [5120, 8], P('tensor'), may hold values from -0.078125 to 0.078125
- gain: bfloat16 [5120], P('tensor'), may hold values from 0.25 to 1.75
- lengths: int32 [512], P('dp'), may hold values from 0 to 63
Outputs:
- uwo: float32 [512], P('dp')
- proj_grad: float32 [5120, 2560], P('dp', 'tensor')
- head_grad: float32 [5120, 8], P('tensor')
- gain_grad: float32 [5120], P('tensor')
The draws below stay inside these ranges and needn't reach their ends.
Inputs may be any that keep to these rules, and one draw needn't show every extreme that they name: Positions 0 to lengths[n] of response n are scored.
All inputs are finite; a program needn't handle non-finite values.
Results may differ from the reference program's by a relative error of at most 0.0085.
Values may be sent and summed in bfloat16 or wider, within the bound.
No kernel may reach another device: no remote copies, remote signals or barrier semaphores. Data moves between devices by JAX's collectives and lax.ppermute only.
A program may use at most 128 MiB of HBM per device.

```python
import jax
import jax.numpy as jnp
from jax import lax

D = 5120
HIN = 2560
HEADS = 8
RESP_DEV = 8
SEQ = 64
RESPONSES = 512
N_DP = 64
N_TENSOR = 4


def plant(entries, own_key, low, high):
    longest = entries.shape.index(max(entries.shape))
    spots = []
    for shift in (0, 1):
        where = [jax.random.randint(jax.random.fold_in(own_key, axis), (), 0, length) for axis, length in enumerate(entries.shape)]
        where[longest] = (where[longest] + shift) % entries.shape[longest]
        spots.append(tuple(where))
    return entries.at[spots[0]].set(low).at[spots[1]].set(high)


def block_scale(stream_key, dims, shards, low, high):
    level = 1.0
    for axis_at, parts in shards:
        heights = jax.random.uniform(jax.random.fold_in(jax.random.fold_in(stream_key, 6), axis_at), (parts,), jnp.float32, low / len(shards), high / len(shards))
        level = level * jnp.repeat(jnp.exp(heights), dims[axis_at] // parts).reshape((-1,) + (1,) * (len(dims) - 1 - axis_at))
    return level


def noise(rng, shape, scale, limit, cuts=(), kind=jnp.bfloat16):
    values = scale * jax.random.normal(rng, shape, jnp.float32)
    if cuts:
        values = values * block_scale(rng, shape, cuts, -0.22, 0.18)
    return jnp.clip(values, -limit, limit).astype(kind)


def setup_inputs(seed: int = 0) -> dict:
    seeds = jax.random.split(jax.random.key(seed), 7)
    attn_out = noise(seeds[0], (RESPONSES * SEQ, HIN), 1.0, 6.0, ((0, 64), (1, 4)))
    resid = noise(seeds[1], (RESPONSES * SEQ, D), 1.0, 6.0, ((0, 64), (1, 4)))
    out_proj = noise(seeds[2], (HIN, D), HIN ** -0.5, 0.125, ((0, 4),))
    heads = noise(seeds[3], (D, HEADS), D ** -0.5, 0.078125, ((0, 4),))
    gain = jnp.clip(1.0 + 0.15 * jax.random.normal(seeds[4], (D,), jnp.float32), 0.25, 1.75).astype(jnp.bfloat16)
    lengths = plant(jax.random.randint(seeds[5], (RESPONSES,), 0, SEQ), jax.random.fold_in(seeds[5], 1), 0, SEQ - 1).astype(jnp.int32)
    return {"attn_out": attn_out, "resid": resid, "out_proj": out_proj, "heads": heads, "gain": gain, "lengths": lengths}


EPS_NORM = 1e-06
EPS_VAR = 1e-05
PENALTY = 0.5

def hidden_rows(attn_block, resid_block, out_proj):
    width = attn_block.shape[1] // N_TENSOR
    total = resid_block.astype(jnp.float32)
    for block in range(N_TENSOR):
        product = jnp.dot(attn_block[:, block * width:(block + 1) * width], out_proj[block * width:(block + 1) * width], preferred_element_type=jnp.float32)
        total = total + lax.optimization_barrier(product.astype(jnp.bfloat16)).astype(jnp.float32)
    return total

def forward_block(attn_block, resid_block, out_proj, heads, gain):
    hidden = hidden_rows(attn_block, resid_block, out_proj)
    rinv = lax.rsqrt(lax.optimization_barrier(jnp.mean(hidden * hidden, axis=1)) + EPS_NORM)
    normed = hidden * rinv[:, None] * gain.astype(jnp.float32)[None, :]
    scores = jnp.dot(normed, heads.astype(jnp.float32), precision=lax.Precision.HIGHEST)
    return (hidden, rinv, normed, scores)

def masks(length_block):
    position = lax.broadcasted_iota(jnp.int32, (length_block.shape[0], SEQ), 1)
    inside = position <= length_block[:, None]
    counts = (length_block + 1).astype(jnp.float32)
    return (inside, counts)

def reference(attn_out, resid, out_proj, heads, gain, lengths):
    attn_blocks = attn_out.reshape(N_DP, RESP_DEV * SEQ, HIN)
    resid_blocks = resid.reshape(N_DP, RESP_DEV * SEQ, D)
    length_blocks = lengths.reshape(N_DP, RESP_DEV)

    def first_pass(items):
        attn_block, resid_block, length_block = items
        scores = forward_block(attn_block, resid_block, out_proj, heads, gain)[3]
        inside, counts = masks(length_block)
        per_resp = scores.reshape(RESP_DEV, SEQ, HEADS)
        summed = lax.optimization_barrier(jnp.sum(jnp.where(inside[:, :, None], per_resp, 0.0), axis=1))
        return summed / counts[:, None]
    rewards = lax.map(first_pass, (attn_blocks, resid_blocks, length_blocks)).reshape(RESPONSES, HEADS)
    center = lax.optimization_barrier(jnp.mean(rewards, axis=0))
    spread = lax.optimization_barrier(jnp.mean((rewards - center[None, :]) ** 2, axis=0))
    zed = (rewards - center[None, :]) * lax.rsqrt(spread + EPS_VAR)[None, :]
    zmean = lax.optimization_barrier(jnp.mean(zed, axis=1))
    uwo = zmean - PENALTY * lax.optimization_barrier(jnp.mean((zed - zmean[:, None]) ** 2, axis=1))
    pairs = rewards.reshape(RESPONSES // 2, 2, HEADS)
    weight = jax.nn.sigmoid(pairs[:, 1] - pairs[:, 0])
    dreward = jnp.stack([-weight, weight], axis=1).reshape(N_DP, RESP_DEV, HEADS)
    gain32 = gain.astype(jnp.float32)
    heads32 = heads.astype(jnp.float32)

    def second_pass(carry, items):
        proj_acc, head_acc, gain_acc = carry
        attn_block, resid_block, length_block, dreward_block = items
        hidden, rinv, normed, scores = forward_block(attn_block, resid_block, out_proj, heads, gain)
        inside, counts = masks(length_block)
        dscore = jnp.where(inside[:, :, None], (dreward_block / counts[:, None])[:, None, :], 0.0).reshape(RESP_DEV * SEQ, HEADS)
        head_acc = head_acc + jnp.dot(normed.T, dscore, precision=lax.Precision.HIGHEST)
        dnormed = jnp.dot(dscore, heads32.T, precision=lax.Precision.HIGHEST)
        gain_acc = gain_acc + lax.optimization_barrier(jnp.sum(dnormed * hidden * rinv[:, None], axis=0))
        inner = lax.optimization_barrier(jnp.sum(hidden * gain32[None, :] * dnormed, axis=1))
        dhidden = (rinv[:, None] * gain32[None, :] * dnormed - hidden * (rinv ** 3 * inner / D)[:, None]).astype(jnp.bfloat16)
        proj_acc = proj_acc + jnp.dot(dhidden.T, attn_block, preferred_element_type=jnp.float32)
        return ((proj_acc, head_acc, gain_acc), None)
    start = (jnp.zeros((D, HIN), jnp.float32), jnp.zeros((D, HEADS), jnp.float32), jnp.zeros((D,), jnp.float32))
    (proj_grad, head_grad, gain_grad), unused = lax.scan(second_pass, start, (attn_blocks, resid_blocks, length_blocks, dreward))
    return (uwo, proj_grad, head_grad, gain_grad)
```

```python
import functools

import jax
import jax.numpy as jnp
from jax import lax
from jax.sharding import Mesh
from jax.sharding import PartitionSpec as P

D = 5120
EPS_NORM = 1e-06
EPS_VAR = 1e-05
PENALTY = 0.5
NX, NZ, NC, NY = 4, 8, 2, 4
HI = lax.Precision.HIGHEST
BF = jnp.bfloat16
F32 = jnp.float32


def shift(x, axis, by):
    n = lax.axis_size(axis)
    return lax.ppermute(x, axis, [(i, (i + by) % n) for i in range(n)])


def butterfly(x, axis):
    n, step = lax.axis_size(axis), 1
    while step < n:
        x = x + lax.ppermute(x, axis, [(i, i ^ step) for i in range(n)])
        step *= 2
    return x


def final_places():
    pairs = []
    for x in range(NX):
        for z in range(NZ):
            for c in range(NC):
                for y in range(NY):
                    src = ((x * NZ + z) * NC + c) * NY + y
                    to = (y, 4 * c + z // 2, z % 2, (y + x) % NY)
                    dst = ((to[0] * NZ + to[1]) * NC + to[2]) * NY + to[3]
                    pairs.append((src, dst))
    return pairs


def gathered_weight(out_proj, x, y, c):
    block = out_proj.shape[0]
    width = out_proj.shape[1] // NY
    half, rows = width // NC, block // NX

    def piece(col, row, n):
        return lax.dynamic_slice(out_proj, (row, col * width + c * half), (n, half))

    mine = piece(y, 0, block)
    parts = jnp.stack([shift(piece((y - r) % NY, x * rows, rows), "y", -r) for r in (1, 2, 3)])
    below, above = shift(parts, "x", 1), shift(parts, "x", -1)
    cut = rows // 2
    far_low, far_high = shift(below[:, :cut], "x", 1), shift(above[:, cut:], "x", -1)
    full = jnp.zeros((3, block, half), out_proj.dtype)
    for part, owner, at in (
        (parts, x, 0),
        (below, (x - 1) % NX, 0),
        (above, (x + 1) % NX, 0),
        (far_low, (x + 2) % NX, 0),
        (far_high, (x + 2) % NX, cut),
    ):
        full = lax.dynamic_update_slice(full, part, (0, owner * rows + at, 0))
    return [mine, full[0], full[1], full[2]]


def gathered_rows(attn):
    cut = attn.shape[0] // 2
    before, after = shift(attn, "y", 1), shift(attn, "y", -1)
    far_low, far_high = shift(before[:cut], "y", 1), shift(after[cut:], "y", -1)
    far = jnp.concatenate([far_low, far_high], axis=0)
    return [jnp.concatenate([a, shift(a, "c", 1)], axis=0) for a in (attn, after, far, before)]


def summed_over_chips(near, up, down, far, x):
    half = far.shape[0] // 2
    came_up = shift(far[:half].astype(BF), "x", 1)
    came_down = shift(far[half:].astype(BF), "x", -1)
    up = jnp.concatenate([up[:half] + came_up.astype(F32), up[half:]], axis=0)
    down = jnp.concatenate([down[:half], down[half:] + came_down.astype(F32)], axis=0)
    total = (
        near
        + shift(up.astype(BF), "x", 1).astype(F32)
        + shift(down.astype(BF), "x", -1).astype(F32)
    )
    blocks = total.astype(BF).reshape(NZ, -1, total.shape[1])
    arrived = lax.all_to_all(blocks, "z", split_axis=0, concat_axis=0, tiled=True)
    total = arrived.astype(F32).sum(axis=0)
    return lax.ppermute(total, ("x", "z", "c", "y"), final_places())


def per_device(attn_out, resid, out_proj, heads, gain, lengths):
    x, c, y = (lax.axis_index(a) for a in ("x", "c", "y"))
    seq = attn_out.shape[0] // lengths.shape[0]
    members = heads.shape[1]
    half = resid.shape[1] // NC

    def own_half(a, axis, which):
        return lax.dynamic_slice_in_dim(a, which * half, half, axis)

    weights = gathered_weight(out_proj, x, y, c)
    rows = gathered_rows(attn_out)
    resid_all = jnp.concatenate(
        [own_half(resid, 1, c), shift(own_half(resid, 1, 1 - c), "c", 1)], axis=0
    )
    lens = jnp.concatenate([lengths, lax.ppermute(lengths.astype(F32), "c", [(0, 1), (1, 0)]).astype(jnp.int32)])
    total_rows, resp = rows[0].shape[0], lens.shape[0]
    gain_own = own_half(gain, 0, c).astype(F32)
    heads_own = own_half(heads, 0, c).astype(F32)
    gain_heads = gain_own[:, None] * heads_own

    hidden = resid_all.astype(F32)
    for a, w in zip(rows, weights):
        hidden = hidden + jnp.dot(a, w, preferred_element_type=F32)
    squares = jnp.sum(hidden * hidden, axis=1)
    raw = jnp.einsum("dk,rd->kr", gain_heads, hidden, precision=HI)
    part = jnp.concatenate([raw, squares[None]], axis=0)
    other = shift(part, "c", 1)
    mid = total_rows // 2
    part = part + jnp.concatenate([other[:, mid:], other[:, :mid]], axis=1)
    part = part + shift(part, "y", 1) + shift(part, "y", -1) + shift(part, "y", 2)
    raw, squares = part[:members], part[members]

    rinv = lax.rsqrt(squares / D + EPS_NORM)
    scores = raw * rinv[None]
    counts = (lens + 1).astype(F32)
    at = lax.broadcasted_iota(jnp.int32, (resp, total_rows), 1) - seq * lax.broadcasted_iota(
        jnp.int32, (resp, total_rows), 0
    )
    inside = ((at >= 0) & (at <= lens[:, None])).astype(F32)
    rewards = jnp.einsum("kr,nr->kn", scores, inside, precision=HI) / counts[None]
    odd = lax.broadcasted_iota(jnp.int32, rewards.shape, 1) % 2 == 1
    partner = jnp.where(odd, jnp.roll(rewards, 1, 1), jnp.roll(rewards, -1, 1))
    sign = jnp.where(odd, 1.0, -1.0)
    dreward = sign * jax.nn.sigmoid(sign * (rewards - partner))
    dscore = jnp.einsum("kn,nr->kr", dreward / counts[None], inside, precision=HI)
    scaled = dscore * rinv[None]
    pull = rinv**3 * jnp.sum(dscore * raw, axis=0) / D
    dhidden = (
        jnp.einsum("kr,dk->rd", scaled, gain_heads, precision=HI) - hidden * pull[:, None]
    ).astype(BF)

    head_term = jnp.einsum("kr,rd->kd", scaled, hidden)
    sums = jnp.stack([jnp.sum(rewards, axis=1), jnp.sum(rewards * rewards, axis=1)], axis=1)
    line = jnp.concatenate([head_term, jnp.pad(sums, ((0, 0), (0, 126)))], axis=1)
    line = butterfly(butterfly(line, "x"), "z")
    head_sum = line[:, :half]
    total_resp = resp * NX * NZ
    center, second = line[:, half] / total_resp, line[:, half + 1] / total_resp
    spread = second - center * center
    zed = ((rewards - center[:, None]) * lax.rsqrt(spread + EPS_VAR)[:, None])[:, : resp // NC]
    zmean = jnp.mean(zed, axis=0)
    uwo = zmean - PENALTY * jnp.mean((zed - zmean[None]) ** 2, axis=0)
    both = shift(head_sum, "c", 1)
    first = c == 0
    whole = jnp.concatenate(
        [jnp.where(first, head_sum, both), jnp.where(first, both, head_sum)], axis=1
    ).T
    head_grad = gain.astype(F32)[:, None] * whole
    gain_grad = jnp.sum(heads.astype(F32) * whole, axis=1)

    stacked = jnp.stack(rows)
    near, up, far, down = (
        lax.dynamic_index_in_dim(stacked, (x + s) % NX, 0, keepdims=False) for s in range(NX)
    )
    proj = []
    width = near.shape[1]
    for lo, hi in ((0, 384), (384, width)):
        terms = [
            jnp.einsum("rd,rj->dj", dhidden, a[:, lo:hi], preferred_element_type=F32)
            for a in (near, up, down, far)
        ]
        proj.append(summed_over_chips(*terms, x))
    return (uwo, jnp.concatenate(proj, axis=1), head_grad, gain_grad)


def solution(mesh):
    finer = Mesh(mesh.devices.reshape(NX, NZ, NC, NY), ("x", "z", "c", "y"))
    dp = ("x", "z", "c")
    in_specs = (P(dp, "y"), P(dp, "y"), P("y", None), P("y", None), P("y"), P(dp))
    out_specs = (P(dp), P(dp, "y"), P("y", None), P("y"))
    return jax.shard_map(
        per_device, mesh=finer, in_specs=in_specs, out_specs=out_specs, check_vma=False
    )
```

```python
import functools

import jax
import jax.numpy as jnp
from jax import lax
from jax.experimental import pallas as pl
from jax.experimental.pallas import tpu as pltpu
from jax.sharding import Mesh
from jax.sharding import PartitionSpec as P

D = 5120
SEQ = 64
EPS_NORM = 1e-06
EPS_VAR = 1e-05
PENALTY = 0.5
NX, NZ, NC, NY = 4, 8, 2, 4
LANES = 128
ROWS = 256
HI = lax.Precision.HIGHEST
BF = jnp.bfloat16
F32 = jnp.float32
SLABS = ((0, 384), (384, 640))


together = lax.optimization_barrier


def shift(x, axis, by):
    n = lax.axis_size(axis)
    return lax.ppermute(x, axis, [(i, (i + by) % n) for i in range(n)])


def butterfly(x, axis):
    n, step = lax.axis_size(axis), 1
    while step < n:
        x = x + lax.ppermute(x, axis, [(i, i ^ step) for i in range(n)])
        step *= 2
    return x


def exchanged(x, axis):
    return lax.all_to_all(x, axis, split_axis=0, concat_axis=0, tiled=True)


def final_places():
    pairs = []
    for x in range(NX):
        for z in range(NZ):
            for c in range(NC):
                for y in range(NY):
                    src = ((x * NZ + z) * NC + c) * NY + y
                    to = (y, 4 * c + z // 2, z % 2, (y + x) % NY)
                    dst = ((to[0] * NZ + to[1]) * NC + to[2]) * NY + to[3]
                    pairs.append((src, dst))
    return pairs


def split(v):
    high = v.astype(BF)
    return high, (v - high.astype(F32)).astype(BF)


def dot_t(a, b):
    return lax.dot_general(a, b, (((1,), (1,)), ((), ())), preferred_element_type=F32)


def hidden_kernel(start, after, far, before, after_c, far_c, before_c, wx, wz, gh, hidden, sums, w):
    xr, zr = wx.shape[2], wz.shape[2]
    for r in range(3):
        for i in range(NX):
            w[r, i * xr : (i + 1) * xr, :] = wx[i, r]
        for i in range(NZ):
            at = NX * xr + i * zr
            w[r, at : at + zr, :] = wz[i, r]
    g_high, g_low = split(gh[...])
    g_both = jnp.concatenate([g_high, g_low], axis=0)
    g_pad = jnp.concatenate([g_high, jnp.zeros_like(g_high)], axis=0)
    ones = jnp.ones(g_both.shape, BF)
    members = g_high.shape[0]
    count = after.shape[0]
    for base, trio in ((0, (after, far, before)), (count, (after_c, far_c, before_c))):

        @pl.loop(0, count // ROWS)
        def _(i):
            here = pl.ds(pl.multiple_of(i * ROWS, ROWS), ROWS)
            there = pl.ds(pl.multiple_of(base + i * ROWS, ROWS), ROWS)
            acc = start[there, :]
            for r in range(3):
                acc += jnp.dot(trio[r][here, :], w[r], preferred_element_type=F32)
            hidden[there, :] = acc
            high, low = split(acc)
            raw = dot_t(g_both, high)
            raw = raw[:members] + raw[members:] + dot_t(g_pad, low)[:members]
            sq_high, sq_low = split(acc * acc)
            squares = dot_t(ones, sq_high) + dot_t(ones, sq_low)
            sums[0:members, there] = raw
            sums[members : 2 * members, there] = squares[:members]


def middle_kernel(p0, p1, p2, p3, lens_row, lens_col, gh, hid, dh_t, line, rew, u_t, scaled_s):
    i = pl.program_id(0)
    members, width = gh.shape

    @pl.when(i == 0)
    def _():
        total = p0[...] + p1[...] + p2[...] + p3[...]
        raw, squares = total[:members], total[members : members + 1]
        rinv = lax.rsqrt(squares / D + EPS_NORM)
        rows = total.shape[1]
        at = lax.broadcasted_iota(jnp.int32, (LANES, rows), 1) - SEQ * lax.broadcasted_iota(
            jnp.int32, (LANES, rows), 0
        )
        inside = ((at >= 0) & (at <= lens_col[:, 0:1])).astype(F32)
        counts = (lens_row[...] + 1).astype(F32)
        rewards = (
            lax.dot_general(
                raw * rinv, inside, (((1,), (1,)), ((), ())), precision=HI, preferred_element_type=F32
            )
            / counts
        )
        lane = lax.broadcasted_iota(jnp.int32, rewards.shape, 1)
        odd = lane % 2 == 1
        partner = jnp.where(odd, pltpu.roll(rewards, 1, 1), pltpu.roll(rewards, LANES - 1, 1))
        sign = jnp.where(odd, 1.0, -1.0)
        dreward = sign * jax.nn.sigmoid(sign * (rewards - partner))
        dscore = jnp.dot(dreward / counts, inside, precision=HI, preferred_element_type=F32)
        scaled = dscore * rinv
        pull = rinv * rinv * rinv * jnp.sum(dscore * raw, axis=0, keepdims=True) / D
        scaled_s[...] = scaled
        u_t[...] = jnp.concatenate([scaled, jnp.broadcast_to(pull, scaled.shape)], axis=0).T
        rew[...] = rewards
        mine = jnp.where(lane < rows // SEQ, rewards, 0.0)
        first = jnp.sum(mine, axis=1, keepdims=True)
        second = jnp.sum(mine * mine, axis=1, keepdims=True)
        line[:, :width] = jnp.zeros((members, width), F32)
        line[:, width:] = jnp.where(lane == 0, first, jnp.where(lane == 1, second, 0.0))

    here = pl.ds(pl.multiple_of(i * ROWS, ROWS), ROWS)
    u = u_t[here, :]
    h = hid[...]
    lift = jnp.dot(u[:, :members], gh[...], precision=HI, preferred_element_type=F32)
    dh_t[...] = (lift - h * u[:, members : members + 1]).T.astype(BF)
    s_high, s_low = split(scaled_s[:, here])
    both = jnp.dot(jnp.concatenate([s_high, s_low], axis=0), h.astype(BF), preferred_element_type=F32)
    line[:, :width] += both[:members] + both[members:]


def whole():
    return pl.BlockSpec(memory_space=pltpu.VMEM)


def hidden_and_sums(start, trio, trio_c, wx, wz, gh):
    rows, width = start.shape
    members = gh.shape[0]
    return pl.pallas_call(
        hidden_kernel,
        out_shape=(
            jax.ShapeDtypeStruct((rows, width), F32),
            jax.ShapeDtypeStruct((2 * members, rows), F32),
        ),
        in_specs=[whole()] * 10,
        out_specs=(whole(), whole()),
        scratch_shapes=[pltpu.VMEM((3, trio[0].shape[1], width), BF)],
        compiler_params=pltpu.CompilerParams(vmem_limit_bytes=32 * 2**20),
        cost_estimate=pl.CostEstimate(
            flops=6 * rows * width * width, bytes_accessed=16 * 2**20, transcendentals=0
        ),
        name="hidden_and_sums",
    )(start, *trio, *trio_c, wx, wz, gh)


def middle(parts, lens, gh, hidden):
    rows, width = hidden.shape
    members = gh.shape[0]
    padded = jnp.pad(lens, (0, LANES - lens.shape[0]))
    fixed = lambda shape: pl.BlockSpec(shape, lambda i: (0, 0))
    return pl.pallas_call(
        middle_kernel,
        grid=(rows // ROWS,),
        out_shape=(
            jax.ShapeDtypeStruct((width, rows), BF),
            jax.ShapeDtypeStruct((members, width + LANES), F32),
            jax.ShapeDtypeStruct((members, LANES), F32),
        ),
        in_specs=[fixed((2 * members, rows))] * 4
        + [
            fixed((1, LANES)),
            fixed((LANES, LANES)),
            fixed((members, width)),
            pl.BlockSpec((ROWS, width), lambda i: (i, 0)),
        ],
        out_specs=(
            pl.BlockSpec((width, ROWS), lambda i: (0, i)),
            fixed((members, width + LANES)),
            fixed((members, LANES)),
        ),
        scratch_shapes=[pltpu.VMEM((rows, 2 * members), F32), pltpu.VMEM((members, rows), F32)],
        compiler_params=pltpu.CompilerParams(vmem_limit_bytes=24 * 2**20),
        cost_estimate=pl.CostEstimate(
            flops=40 * rows * width, bytes_accessed=6 * 2**20, transcendentals=0
        ),
        name="middle",
    )(*parts, padded[None], jnp.broadcast_to(padded[:, None], (LANES, LANES)), gh, hidden)


def gathered_weight(out_proj, x, z, y, c):
    block = out_proj.shape[0]
    half = out_proj.shape[1] // (NY * NC)
    zr = 24
    xr = (block - NZ * zr) // NX
    picked = jnp.concatenate(
        [
            lax.dynamic_slice_in_dim(out_proj, x * xr, xr, 0),
            lax.dynamic_slice_in_dim(out_proj, NX * xr + z * zr, zr, 0),
        ],
        axis=0,
    )
    sent = jnp.stack(
        [lax.dynamic_slice_in_dim(picked, (2 * k + c) * half, half, 1) for k in range(NY)]
    )
    came = exchanged(sent, "y")
    ahead = jnp.stack(
        [lax.dynamic_index_in_dim(came, (y + r) % NY, 0, keepdims=False) for r in (1, 2, 3)]
    )

    def to_all(a, axis):
        return exchanged(jnp.broadcast_to(a[None], (lax.axis_size(axis), *a.shape)), axis)

    return to_all(ahead[:, :xr], "x"), to_all(ahead[:, xr:], "z")


def per_device(attn_out, resid, out_proj, heads, gain, lengths):
    x, z, c, y = (lax.axis_index(a) for a in ("x", "z", "c", "y"))
    count, block = attn_out.shape
    members = heads.shape[1]
    half = resid.shape[1] // NC

    def own_half(a, axis, which):
        return lax.dynamic_slice_in_dim(a, which * half, half, axis)

    wx, wz = gathered_weight(out_proj, x, z, y, c)
    before, after = shift(attn_out, "y", 1), shift(attn_out, "y", -1)
    cut = count // 2
    far = jnp.concatenate([shift(before[:cut], "y", 1), shift(after[cut:], "y", -1)], axis=0)
    lens_row = jnp.zeros((8, block), BF).at[0, : lengths.shape[0]].set(lengths.astype(BF))
    pack = shift(jnp.concatenate([attn_out, own_half(resid, 1, 1 - c), lens_row], axis=0), "c", 1)
    trio = (after, far, before)
    trio_c = tuple(shift(a, "c", 1) for a in trio)
    lens = jnp.concatenate([lengths, pack[2 * count, : lengths.shape[0]].astype(jnp.int32)])
    resp = lens.shape[0]
    gh = (own_half(gain, 0, c).astype(F32)[:, None] * own_half(heads, 0, c).astype(F32)).T

    own_rows = jnp.concatenate([attn_out, pack[:count]], axis=0)
    mine = lax.dynamic_slice_in_dim(out_proj, (2 * y + c) * half, half, 1)
    start = jnp.concatenate([own_half(resid, 1, c), pack[count : 2 * count]], axis=0).astype(
        F32
    ) + jnp.dot(own_rows, mine, preferred_element_type=F32)
    hidden, part = hidden_and_sums(start, trio, trio_c, wx, wz, gh)

    other = shift(part, "c", 1)
    part = part + jnp.concatenate([other[:, count:], other[:, :count]], axis=1)
    parts = (part, shift(part, "y", 1), shift(part, "y", -1), shift(part, "y", 2))
    dh_t, line, rewards = middle(parts, lens, gh, hidden)

    stacked = jnp.stack(
        [own_rows] + [jnp.concatenate([a, b], axis=0) for a, b in zip(trio, trio_c)]
    )
    near_a, up_a, far_a, down_a = together(
        tuple(lax.dynamic_index_in_dim(stacked, (x + s) % NX, 0, keepdims=False) for s in range(NX))
    )
    cut = half // 2

    def term(lhs, rhs, lo, hi):
        return jnp.dot(lhs, rhs[:, lo:hi], preferred_element_type=F32)

    came = []
    for lo, hi in SLABS:
        top = term(dh_t[:cut], far_a, lo, hi).astype(BF)
        low = term(dh_t[cut:], far_a, lo, hi).astype(BF)
        came.append((shift(top, "x", 1), shift(low, "x", -1)))
    terms = together(
        tuple(tuple(term(dh_t, a, lo, hi) for a in (near_a, up_a, down_a)) for lo, hi in SLABS)
    )
    proj = []
    for (near, up, down), (came_up, came_down) in zip(terms, came):
        up = jnp.concatenate([up[:cut] + came_up.astype(F32), up[cut:]], axis=0)
        down = jnp.concatenate([down[:cut], down[cut:] + came_down.astype(F32)], axis=0)
        got_up, got_down = shift(up.astype(BF), "x", 1), shift(down.astype(BF), "x", -1)
        total = near + got_up.astype(F32) + got_down.astype(F32)
        arrived = exchanged(total.astype(BF).reshape(NZ, -1, total.shape[1]), "z")
        total = arrived.astype(F32).sum(axis=0)
        proj.append(lax.ppermute(total, ("x", "z", "c", "y"), final_places()))

    line = together((line, came))[0]
    line = butterfly(butterfly(line, "x"), "z")
    head_sum = line[:, :half]
    total_resp = resp * NX * NZ
    center, second = line[:, half] / total_resp, line[:, half + 1] / total_resp
    spread = second - center * center
    zed = (rewards[:, : resp // NC] - center[:, None]) * lax.rsqrt(spread + EPS_VAR)[:, None]
    zmean = jnp.mean(zed, axis=0)
    uwo = zmean - PENALTY * jnp.mean((zed - zmean[None]) ** 2, axis=0)
    both = shift(head_sum, "c", 1)
    first = c == 0
    whole_sum = jnp.concatenate(
        [jnp.where(first, head_sum, both), jnp.where(first, both, head_sum)], axis=1
    ).T
    head_grad = gain.astype(F32)[:, None] * whole_sum
    gain_grad = jnp.sum(heads.astype(F32) * whole_sum, axis=1)
    return (uwo, jnp.concatenate(proj, axis=1), head_grad, gain_grad)


def solution(mesh):
    finer = Mesh(mesh.devices.reshape(NX, NZ, NC, NY), ("x", "z", "c", "y"))
    dp = ("x", "z", "c")
    in_specs = (P(dp, "y"), P(dp, "y"), P("y", None), P("y", None), P("y"), P(dp))
    out_specs = (P(dp), P(dp, "y"), P("y", None), P("y"))
    return jax.shard_map(
        per_device, mesh=finer, in_specs=in_specs, out_specs=out_specs, check_vma=False
    )
```

```python
import jax
import jax.numpy as jnp
from jax import lax
from jax.experimental import pallas as pl
from jax.experimental.pallas import tpu as pltpu
from jax.sharding import Mesh
from jax.sharding import PartitionSpec as P

D = 5120
SEQ = 64
EPS_NORM = 1e-06
EPS_VAR = 1e-05
PENALTY = 0.5
NX, NZ, NC, NY = 4, 8, 2, 4
LANES = 128
ROWS = 256
MIB = 2**20
HI = lax.Precision.HIGHEST
BF = jnp.bfloat16
F32 = jnp.float32


together = lax.optimization_barrier


def exchanged(x, axis):
    return lax.all_to_all(x, axis, split_axis=0, concat_axis=0, tiled=True)


def shift(x, axis, by):
    n = lax.axis_size(axis)
    return lax.ppermute(x, axis, [(i, (i + by) % n) for i in range(n)])


def other_core(x):
    return lax.ppermute(x, "c", [(0, 1), (1, 0)])


def shift_by_core(x, axis):
    n = lax.axis_size(axis)
    moves = [(c, i, (i + 1 - 2 * c) % n) for c in range(NC) for i in range(n)]
    if axis == "y":
        return lax.ppermute(x, ("c", axis), [(c * n + i, c * n + j) for c, i, j in moves])
    return lax.ppermute(x, (axis, "c"), [(i * NC + c, j * NC + c) for c, i, j in moves])


def chunk_of(z, c):
    if c == 0:
        return 2 * z if z < NZ // 2 else 2 * (NZ - 1 - z) + 1
    return 2 * (z - NZ // 2) + 1 if z >= NZ // 2 else 2 * (NZ // 2 - 1 - z)


def final_places():
    pairs = []
    for x in range(NX):
        for z in range(NZ):
            for c in range(NC):
                for y in range(NY):
                    src = ((x * NZ + z) * NC + c) * NY + y
                    q = chunk_of(z, c)
                    dst = ((y * NZ + 4 * c + q // 2) * NC + q % 2) * NY + (y + x) % NY
                    pairs.append((src, dst))
    return pairs


def in_pieces(v, count):
    pieces = []
    for _ in range(count):
        high = lax.reduce_precision(v, 8, 7)
        pieces.append(high.astype(BF))
        v = v - high
    return pieces


def as_rows(line, sums, line_count):
    small = jnp.concatenate(in_pieces(sums, 3), axis=1)
    small = jnp.pad(small, ((0, 0), (0, line.shape[1] - small.shape[1])))
    return jnp.concatenate([*in_pieces(line, line_count), small], axis=0)


def from_rows(rows, members, line_count):
    rows = rows.astype(F32)
    line = sum(rows[i * members : (i + 1) * members] for i in range(line_count))
    small = rows[line_count * members :, :6]
    return line, small[:, 0:2] + small[:, 2:4] + small[:, 4:6]


def gathered_weight(out_proj, x, y, c):
    block = out_proj.shape[0]
    half = out_proj.shape[1] // (NY * NC)
    rows = block // NX
    picked = lax.dynamic_slice_in_dim(out_proj, x * rows, rows, 0)
    sent = jnp.stack(
        [lax.dynamic_slice_in_dim(picked, (2 * k + c) * half, half, 1) for k in range(NY)]
    )
    came = exchanged(sent, "y")
    own = jnp.stack(
        [lax.dynamic_index_in_dim(came, (y + r) % NY, 0, keepdims=False) for r in (1, 2, 3)]
    )
    low, high = shift(own, "x", 1), shift(own, "x", -1)
    low, high, onward = together((low, high, jnp.where(c == 0, low, high)))
    far = shift_by_core(onward, "x")
    return sent, (own, low, high, far)


def split(v):
    high = v.astype(BF)
    return high, (v - high.astype(F32)).astype(BF)


def dot(a, b):
    return jnp.dot(a, b, preferred_element_type=F32)


def hidden_kernel(where, *refs):
    rows, refs = refs[: NC * NY], refs[NC * NY :]
    out_proj, w_own, w_low, w_high, w_far, resid, pack, gh, hidden, sums, *refs = refs
    turned, (a, w, mine, res, sem) = refs[:NX], refs[NX:]
    y, c, x = where[0], where[1], where[2]
    count, half = rows[0].shape
    part = w_own.shape[1]
    halves = (slice(0, count), slice(count, 2 * count))
    columns = lambda i: pl.ds(pl.multiple_of(i * half, LANES), half)
    copies = []

    def fetch(src, dst):
        copies.append(pltpu.make_async_copy(src, dst, sem.at[len(copies)]))
        copies[-1].start()
        return copies[-1]

    first = [fetch(out_proj.at[:, columns(2 * y + c)], mine)]
    for i, (r, h) in enumerate(zip((resid.at[:, columns(c)], pack.at[halves[0], :]), halves)):
        first += [fetch(r, res.at[h, :]), fetch(rows[i], a.at[0, h, :])]
    pieces = []
    for piece, owner in ((w_own, x), (w_low, x + NX - 1), (w_high, x + 1), (w_far, x + 2)):
        at = pl.ds(pl.multiple_of(lax.rem(owner, NX) * part, part), part)
        pieces.append(fetch(piece, w.at[:, at, :]))
    later = [
        fetch(rows[NC * r + i], a.at[r, h, :]) for r in range(1, NY) for i, h in enumerate(halves)
    ]
    blocks = NC * count // ROWS
    g_high, g_low = split(gh[...])
    lane = lax.broadcasted_iota(jnp.int32, (ROWS, LANES), 1)
    members = sums.shape[0] // 2

    for copy in first:
        copy.wait()

    @pl.loop(0, blocks)
    def _(i):
        here = pl.ds(pl.multiple_of(i * ROWS, ROWS), ROWS)
        hidden[here, :] = res[here, :].astype(F32) + dot(a[0, here, :], mine[...])

    for copy in pieces + later:
        copy.wait()
    moved = [fetch(a.at[lax.rem(x + s, NX)], turned[s]) for s in range(NX)]

    @pl.loop(0, blocks)
    def _(i):
        here = pl.ds(pl.multiple_of(i * ROWS, ROWS), ROWS)
        acc = hidden[here, :]
        for r in range(1, NY):
            acc += dot(a[r, here, :], w[r - 1])
        hidden[here, :] = acc
        high, low = split(acc)
        tile = dot(high, g_high) + dot(high, g_low) + dot(low, g_high)
        squares = jnp.sum(acc * acc, axis=1, keepdims=True)
        tile = jnp.where(lane == members, squares, tile).T
        sums[:, here] = tile[: 2 * members]

    for copy in moved:
        copy.wait()


def hidden_and_sums(where, rows, out_proj, weights, resid, pack, gh):
    count, half = rows[0].shape
    members = gh.shape[1]
    total = NC * count
    gh = jnp.pad(gh, ((0, 0), (0, LANES - members)))
    any_space = pl.BlockSpec(memory_space=pl.ANY)
    full = lambda shape: pl.BlockSpec(shape, lambda i, s: (0, 0))
    return pl.pallas_call(
        hidden_kernel,
        grid_spec=pltpu.PrefetchScalarGridSpec(
            num_scalar_prefetch=1,
            grid=(1,),
            in_specs=[any_space] * (NC * NY + 7) + [full(gh.shape)],
            out_specs=[full((total, half)), full((2 * members, total))] + [pl.BlockSpec(memory_space=pltpu.HBM)] * NX,
            scratch_shapes=[
                pltpu.VMEM((NY, total, half), BF),
                pltpu.VMEM((NY - 1, half, half), BF),
                pltpu.VMEM((half, half), BF),
                pltpu.VMEM((total, half), BF),
                pltpu.SemaphoreType.DMA((NC * NY + 7 + NX,)),
            ],
        ),
        out_shape=[
            jax.ShapeDtypeStruct((total, half), F32),
            jax.ShapeDtypeStruct((2 * members, total), F32),
        ]
        + [jax.ShapeDtypeStruct((total, half), BF)] * NX,
        compiler_params=pltpu.CompilerParams(vmem_limit_bytes=40 * MIB),
        cost_estimate=pl.CostEstimate(
            flops=8 * total * half * half, bytes_accessed=20 * MIB, transcendentals=0
        ),
        name="hidden_and_sums",
    )(where, *rows, out_proj, *weights, resid, pack, gh)


def per_device(attn_out, resid, out_proj, heads, gain, lengths):
    x, c, y = (lax.axis_index(a) for a in ("x", "c", "y"))
    count, block = attn_out.shape
    members = heads.shape[1]
    half = resid.shape[1] // NC
    resp_own = lengths.shape[0]
    first = c == 0

    def own_half(a, axis, which):
        return lax.dynamic_slice_in_dim(a, which * half, half, axis)

    sent, weights = gathered_weight(out_proj, x, y, c)
    attn = together((attn_out, sent))[0]
    before, after = shift(attn, "y", 1), shift(attn, "y", -1)
    before, after, onward, resid_other = together(
        (before, after, jnp.where(first, before, after), resid)
    )
    far = shift_by_core(onward, "y")
    rows = [b for a in (attn, after, far, before) for b in (a, other_core(a))]
    lens_rows = jnp.zeros((8, half), BF).at[0, :resp_own].set(lengths.astype(BF))
    pack = other_core(jnp.concatenate([own_half(resid_other, 1, 1 - c), lens_rows], axis=0))
    lens = jnp.concatenate([lengths, pack[count, :resp_own].astype(jnp.int32)])
    total_rows, resp = 2 * count, 2 * resp_own
    gain_heads = own_half(gain, 0, c).astype(F32)[:, None] * own_half(heads, 0, c).astype(F32)
    where = jnp.stack([y, c, x]).astype(jnp.int32)
    hidden, part, near_a, up_a, far_a, down_a = hidden_and_sums(
        where, rows, out_proj, weights, resid, pack, gain_heads
    )
    other = other_core(part)
    part = part + jnp.concatenate([other[:, count:], other[:, :count]], axis=1)
    part = part + shift(part, "y", 1) + shift(part, "y", -1) + shift(part, "y", 2)
    raw, squares = part[:members], part[members]

    rinv = lax.rsqrt(squares / D + EPS_NORM)
    scores = raw * rinv[None]
    counts = (lens + 1).astype(F32)
    at = lax.broadcasted_iota(jnp.int32, (resp, total_rows), 1) - SEQ * lax.broadcasted_iota(
        jnp.int32, (resp, total_rows), 0
    )
    inside = ((at >= 0) & (at <= lens[:, None])).astype(F32)
    rewards = jnp.einsum("kr,nr->kn", scores, inside, precision=HI) / counts[None]
    odd = lax.broadcasted_iota(jnp.int32, rewards.shape, 1) % 2 == 1
    partner = jnp.where(odd, jnp.roll(rewards, 1, 1), jnp.roll(rewards, -1, 1))
    sign = jnp.where(odd, 1.0, -1.0)
    dreward = sign * jax.nn.sigmoid(sign * (rewards - partner))
    dscore = jnp.einsum("kn,nr->kr", dreward / counts[None], inside, precision=HI)
    scaled = dscore * rinv[None]
    pull = rinv**3 * jnp.sum(dscore * raw, axis=0) / D
    dhidden = (
        jnp.einsum("kr,dk->rd", scaled, gain_heads, precision=HI) - hidden * pull[:, None]
    ).astype(BF)
    line = jnp.einsum("kr,rd->kd", scaled, hidden)
    sums = jnp.stack([jnp.sum(rewards, axis=1), jnp.sum(rewards * rewards, axis=1)], axis=1)

    def term(a):
        return jnp.einsum("rd,rj->dj", dhidden, a, preferred_element_type=F32)

    outward = together(
        (jnp.concatenate([term(far_a).astype(BF), as_rows(line, sums, 2)], axis=0), dhidden)
    )
    came, dhidden = shift_by_core(outward[0], "x"), outward[1]
    near, up, down = together((term(near_a), term(up_a), term(down_a)))
    arrived = came[:half].astype(F32)
    came_line, came_sums = from_rows(came[half:], members, 2)

    def passed_on(t, use):
        extra = as_rows(
            line + jnp.where(use, came_line, 0.0), sums + jnp.where(use, came_sums, 0.0), 2
        )
        return jnp.concatenate([(t + jnp.where(use, arrived, 0.0)).astype(BF), extra], axis=0)

    got_up = shift(passed_on(up, first), "x", 1)
    got_down = shift(passed_on(down, ~first), "x", -1)
    total = (near + got_up[:half].astype(F32) + got_down[:half].astype(F32)).astype(BF)
    up_line, up_sums = from_rows(got_up[half:], members, 2)
    down_line, down_sums = from_rows(got_down[half:], members, 2)
    extra = as_rows(line + up_line + down_line, sums + up_sums + down_sums, 1)
    total = total.reshape(NZ, -1, block)
    orders = [jnp.stack([total[chunk_of(z, k)] for z in range(NZ)]) for k in range(NC)]
    blocks = jnp.concatenate(
        [
            jnp.where(first, *orders),
            jnp.broadcast_to(extra[None], (NZ, *extra.shape)),
        ],
        axis=1,
    )
    done = exchanged(blocks, "z").astype(F32).sum(axis=0)
    chunk = half // NZ
    proj = lax.ppermute(done[:chunk].astype(BF), ("x", "z", "c", "y"), final_places()).astype(F32)
    head_sum, reward_sums = from_rows(done[chunk:], members, 1)
    both = other_core(head_sum)
    whole_sum = jnp.concatenate(
        [jnp.where(first, head_sum, both), jnp.where(first, both, head_sum)], axis=1
    ).T
    head_grad = gain.astype(F32)[:, None] * whole_sum
    gain_grad = jnp.sum(heads.astype(F32) * whole_sum, axis=1)

    reward_sums = reward_sums / (resp * NX * NZ)
    center, second = reward_sums[:, 0], reward_sums[:, 1]
    spread = second - center * center
    zed = (rewards[:, :resp_own] - center[:, None]) * lax.rsqrt(spread + EPS_VAR)[:, None]
    zmean = jnp.mean(zed, axis=0)
    uwo = zmean - PENALTY * jnp.mean((zed - zmean[None]) ** 2, axis=0)
    return (uwo, proj, head_grad, gain_grad)


def solution(mesh):
    finer = Mesh(mesh.devices.reshape(NX, NZ, NC, NY), ("x", "z", "c", "y"))
    dp = ("x", "z", "c")
    in_specs = (P(dp, "y"), P(dp, "y"), P("y", None), P("y", None), P("y"), P(dp))
    out_specs = (P(dp), P(dp, "y"), P("y", None), P("y"))
    return jax.shard_map(
        per_device, mesh=finer, in_specs=in_specs, out_specs=out_specs, check_vma=False
    )
```

```python
import jax
import jax.numpy as jnp
from jax import lax
from jax.experimental import pallas as pl
from jax.experimental.pallas import tpu as pltpu
from jax.sharding import Mesh
from jax.sharding import PartitionSpec as P

D = 5120
SEQ = 64
EPS_NORM = 1e-06
EPS_VAR = 1e-05
PENALTY = 0.5
NX, NZ, NC, NY = 4, 8, 2, 4
LANES = 128
CUT = 256
ROWS = 256
MIB = 2**20
HI = lax.Precision.HIGHEST
BF = jnp.bfloat16
F32 = jnp.float32


together = lax.optimization_barrier


def exchanged(x, axis):
    return lax.all_to_all(x, axis, split_axis=0, concat_axis=0, tiled=True)


def shift(x, axis, by):
    n = lax.axis_size(axis)
    return lax.ppermute(x, axis, [(i, (i + by) % n) for i in range(n)])


def other_core(x):
    return lax.ppermute(x, "c", [(0, 1), (1, 0)])


def shift_by_core(x, axis):
    n = lax.axis_size(axis)
    moves = [(c, i, (i + 1 - 2 * c) % n) for c in range(NC) for i in range(n)]
    if axis == "y":
        return lax.ppermute(x, ("c", axis), [(c * n + i, c * n + j) for c, i, j in moves])
    return lax.ppermute(x, (axis, "c"), [(i * NC + c, j * NC + c) for c, i, j in moves])


def chunk_of(z, c):
    if c == 0:
        return 2 * z if z < NZ // 2 else 2 * (NZ - 1 - z) + 1
    return 2 * (z - NZ // 2) + 1 if z >= NZ // 2 else 2 * (NZ // 2 - 1 - z)


def final_places():
    pairs = []
    for x in range(NX):
        for z in range(NZ):
            for c in range(NC):
                for y in range(NY):
                    src = ((x * NZ + z) * NC + c) * NY + y
                    q = chunk_of(z, c)
                    dst = ((y * NZ + 4 * c + q // 2) * NC + q % 2) * NY + (y + x) % NY
                    pairs.append((src, dst))
    return pairs


def in_pieces(v, count):
    pieces = []
    for _ in range(count):
        high = lax.reduce_precision(v, 8, 7)
        pieces.append(high.astype(BF))
        v = v - high
    return pieces


def line_rows(line, count):
    return jnp.concatenate(in_pieces(line, count), axis=0)


def rows_line(rows, members):
    rows = rows.astype(F32)
    return sum(rows[i : i + members] for i in range(0, rows.shape[0], members))


def sum_rows(sums):
    small = jnp.concatenate(in_pieces(sums, 3), axis=1)
    return jnp.pad(small, ((0, 0), (0, LANES - small.shape[1])))


def rows_sum(rows):
    small = rows[:, :6].astype(F32)
    return small[:, 0:2] + small[:, 2:4] + small[:, 4:6]


def gathered_weight(out_proj, x, y, c):
    block = out_proj.shape[0]
    half = out_proj.shape[1] // (NY * NC)
    rows = block // NX
    picked = lax.dynamic_slice_in_dim(out_proj, x * rows, rows, 0)
    sent = jnp.stack(
        [lax.dynamic_slice_in_dim(picked, (2 * k + c) * half, half, 1) for k in range(NY)]
    )
    came = exchanged(sent, "y")
    own = jnp.stack(
        [lax.dynamic_index_in_dim(came, (y + r) % NY, 0, keepdims=False) for r in (1, 2, 3)]
    )
    low, high = shift(own, "x", 1), shift(own, "x", -1)
    low, high, onward = together((low, high, jnp.where(c == 0, low, high)))
    far = shift_by_core(onward, "x")
    return sent, (own, low, high, far)


def split(v):
    high = v.astype(BF)
    return high, (v - high.astype(F32)).astype(BF)


def dot(a, b):
    return jnp.dot(a, b, preferred_element_type=F32)


def hidden_kernel(where, *refs):
    rows, refs = refs[: NC * NY], refs[NC * NY :]
    out_proj, w_own, w_low, w_high, w_far, resid, pack, gh, hidden, sums, *refs = refs
    turned, a, w, res, sem = refs
    y, c, x = where[0], where[1], where[2]
    count, half = rows[0].shape
    part = w_own.shape[1]
    halves = (slice(0, count), slice(count, 2 * count))
    columns = lambda i: pl.ds(pl.multiple_of(i * half, LANES), half)
    copies = []

    def fetch(src, dst):
        copies.append(pltpu.make_async_copy(src, dst, sem.at[len(copies)]))
        copies[-1].start()
        return copies[-1]

    ready = [fetch(out_proj.at[:, columns(2 * y + c)], w.at[0])]
    for piece, owner in ((w_own, x), (w_low, x + NX - 1), (w_high, x + 1), (w_far, x + 2)):
        at = pl.ds(pl.multiple_of(lax.rem(owner, NX) * part, part), part)
        ready.append(fetch(piece, w.at[1:NY, at, :]))
    for i, r in enumerate((resid.at[:, columns(c)], pack.at[halves[0], :])):
        ready.append(fetch(r, res.at[halves[i], :]))
        for k in range(NY):
            ready.append(fetch(rows[NC * k + i], a.at[halves[i], k * half : (k + 1) * half]))
    early = len(ready) - NY - 1
    blocks = count // ROWS
    g_high, g_low = split(gh[...])
    lane = lax.broadcasted_iota(jnp.int32, (ROWS, LANES), 1)
    members = sums.shape[0] // 2

    def multiply(base):
        @pl.loop(0, blocks)
        def _(i):
            here = pl.ds(pl.multiple_of(base + i * ROWS, ROWS), ROWS)
            acc = res[here, :].astype(F32) + dot(a[here, :], w[...].reshape(NY * half, half))
            hidden[here, :] = acc
            high, low = split(acc)
            tile = dot(high, g_high) + dot(high, g_low) + dot(low, g_high)
            squares = jnp.sum(acc * acc, axis=1, keepdims=True)
            tile = jnp.where(lane == members, squares, tile).T
            sums[:, here] = tile[: 2 * members]

    for copy in ready[:early]:
        copy.wait()
    multiply(0)
    for copy in ready[early:]:
        copy.wait()
    moved = [
        fetch(a.at[:, columns(lax.rem(x + s, NX))], turned.at[s * NC * count : (s + 1) * NC * count])
        for s in range(NX)
    ]
    multiply(count)
    for copy in moved:
        copy.wait()


def hidden_and_sums(where, rows, out_proj, weights, resid, pack, gh):
    count, half = rows[0].shape
    members = gh.shape[1]
    total = NC * count
    gh = jnp.pad(gh, ((0, 0), (0, LANES - members)))
    any_space = pl.BlockSpec(memory_space=pl.ANY)
    full = lambda shape: pl.BlockSpec(shape, lambda i, s: (0, 0))
    return pl.pallas_call(
        hidden_kernel,
        grid_spec=pltpu.PrefetchScalarGridSpec(
            num_scalar_prefetch=1,
            grid=(1,),
            in_specs=[any_space] * (NC * NY + 7) + [full(gh.shape)],
            out_specs=[full((total, half)), full((2 * members, total)), any_space],
            scratch_shapes=[
                pltpu.VMEM((total, NY * half), BF),
                pltpu.VMEM((NY, half, half), BF),
                pltpu.VMEM((total, half), BF),
                pltpu.SemaphoreType.DMA((NC * NY + 7 + NX,)),
            ],
        ),
        out_shape=[
            jax.ShapeDtypeStruct((total, half), F32),
            jax.ShapeDtypeStruct((2 * members, total), F32),
            jax.ShapeDtypeStruct((NX * total, half), BF),
        ],
        compiler_params=pltpu.CompilerParams(vmem_limit_bytes=40 * MIB),
        cost_estimate=pl.CostEstimate(
            flops=8 * total * half * half, bytes_accessed=20 * MIB, transcendentals=0
        ),
        name="hidden_and_sums",
    )(where, *rows, out_proj, *weights, resid, pack, gh)


def step(attn_out, resid, out_proj, heads, gain, lengths):
    x, c, y = (lax.axis_index(a) for a in ("x", "c", "y"))
    count, _ = attn_out.shape
    members = heads.shape[1]
    half = resid.shape[1] // NC
    resp_own = lengths.shape[0]
    first = c == 0

    def own_half(a, axis, which):
        return lax.dynamic_slice_in_dim(a, which * half, half, axis)

    sent, weights = gathered_weight(out_proj, x, y, c)
    attn = together((attn_out, sent))[0]
    before, after = shift(attn, "y", 1), shift(attn, "y", -1)
    before, after, onward, resid_other = together(
        (before, after, jnp.where(first, before, after), resid)
    )
    far = shift_by_core(onward, "y")
    rows = [b for a in (attn, after, far, before) for b in (a, other_core(a))]
    lens_rows = jnp.zeros((8, half), BF).at[0, :resp_own].set(lengths.astype(BF))
    pack = other_core(jnp.concatenate([own_half(resid_other, 1, 1 - c), lens_rows], axis=0))
    lens = jnp.concatenate([lengths, pack[count, :resp_own].astype(jnp.int32)])
    total_rows, resp = 2 * count, 2 * resp_own
    gain_heads = own_half(gain, 0, c).astype(F32)[:, None] * own_half(heads, 0, c).astype(F32)
    where = jnp.stack([y, c, x]).astype(jnp.int32)
    hidden, part, turned = hidden_and_sums(
        where, rows, out_proj, weights, resid, pack, gain_heads
    )
    other = other_core(part)
    part = part + jnp.concatenate([other[:, count:], other[:, :count]], axis=1)
    part = part + shift(part, "y", 1) + shift(part, "y", -1) + shift(part, "y", 2)
    raw, squares = part[:members], part[members]

    rinv = lax.rsqrt(squares / D + EPS_NORM)
    scores = raw * rinv[None]
    counts = (lens + 1).astype(F32)
    at = lax.broadcasted_iota(jnp.int32, (resp, total_rows), 1) - SEQ * lax.broadcasted_iota(
        jnp.int32, (resp, total_rows), 0
    )
    inside = ((at >= 0) & (at <= lens[:, None])).astype(F32)
    rewards = jnp.einsum("kr,nr->kn", scores, inside, precision=HI) / counts[None]
    odd = lax.broadcasted_iota(jnp.int32, rewards.shape, 1) % 2 == 1
    partner = jnp.where(odd, jnp.roll(rewards, 1, 1), jnp.roll(rewards, -1, 1))
    sign = jnp.where(odd, 1.0, -1.0)
    dreward = sign * jax.nn.sigmoid(sign * (rewards - partner))
    dscore = jnp.einsum("kn,nr->kr", dreward / counts[None], inside, precision=HI)
    scaled = dscore * rinv[None]
    pull = rinv**3 * jnp.sum(dscore * raw, axis=0) / D
    dhidden = (
        jnp.einsum("kr,dk->rd", scaled, gain_heads, precision=HI) - hidden * pull[:, None]
    ).astype(BF)
    line = jnp.einsum("kr,rd->kd", scaled, hidden)
    sums = jnp.stack([jnp.sum(rewards, axis=1), jnp.sum(rewards * rewards, axis=1)], axis=1)

    near_a, up_a, far_a, down_a = (
        turned[s * total_rows : (s + 1) * total_rows] for s in range(NX)
    )

    def term(left, right):
        return jnp.einsum("rd,rj->dj", left, right, preferred_element_type=F32)

    slabs = (slice(CUT, None), slice(0, CUT))
    lines = [line[:, lanes] for lanes in slabs]
    extras = [sums, None]

    def with_rows(body, head, extra, count):
        rows = [body, line_rows(head, count)]
        if extra is not None:
            rows.append(jnp.pad(sum_rows(extra), ((0, 0), (0, body.shape[-1] - LANES))))
        return jnp.concatenate(rows, axis=0)

    def read_rows(rows, extra):
        if extra is None:
            return rows_line(rows, members), None
        return rows_line(rows[:-members], members), rows_sum(rows[-members:])

    came = []
    for lanes, head, extra in zip(slabs, lines, extras):
        outward = with_rows(term(dhidden, far_a[:, lanes]).astype(BF), head, extra, 2)
        outward, dhidden = together((outward, dhidden))
        came.append(shift_by_core(outward, "x"))
    near, up, down = together(tuple(term(dhidden, t) for t in (near_a, up_a, down_a)))

    sends = []
    for lanes, head, extra, got in zip(slabs, lines, extras, came):
        arrived = got[:half].astype(F32)
        got_head, got_extra = read_rows(got[half:], extra)

        def passed_on(t, use):
            body = (t[:, lanes] + jnp.where(use, arrived, 0.0)).astype(BF)
            more = None if extra is None else extra + jnp.where(use, got_extra, 0.0)
            return with_rows(body, head + jnp.where(use, got_head, 0.0), more, 2)

        pair = together((passed_on(up, first), passed_on(down, ~first)))
        got_up = shift(pair[0], "x", 1)
        got_down = shift(pair[1], "x", -1)
        sends.append((got_up, got_down))

    chunk = half // NZ
    totals = []
    for lanes, head, extra, (got_up, got_down) in zip(slabs, lines, extras, sends):
        body = near[:, lanes] + got_up[:half].astype(F32) + got_down[:half].astype(F32)
        up_head, up_extra = read_rows(got_up[half:], extra)
        down_head, down_extra = read_rows(got_down[half:], extra)
        head = head + up_head + down_head
        more = None if extra is None else extra + up_extra + down_extra
        totals.append(together((body.astype(BF), head, more)))

    body, head, extra = totals[0]
    rows = with_rows(body[:0], head, extra, 1)
    body = body.reshape(NZ, chunk, -1)
    orders = [jnp.stack([body[chunk_of(k, core)] for k in range(NZ)]) for core in range(NC)]
    blocks = jnp.concatenate(
        [jnp.where(first, *orders), jnp.broadcast_to(rows[None], (NZ, *rows.shape))], axis=1
    )
    done = exchanged(blocks, "z")
    done = done.astype(F32).sum(axis=0)
    head_0, reward_sums = read_rows(done[chunk:].astype(F32), extra)

    body, head, extra = totals[1]
    rows = line_rows(head, 1)

    def chunk_for(to):
        low = jnp.where(first, 2 * to, 2 * (NZ // 2 - 1 - to))
        high = jnp.where(first, 2 * (NZ - 1 - to) + 1, 2 * (to - NZ // 2) + 1)
        at = jnp.where(to < NZ // 2, low, high) * chunk
        return jnp.concatenate([lax.dynamic_slice_in_dim(body, at, chunk, 0), rows], axis=0)

    z = lax.axis_index("z")
    last = chunk_for(z).astype(F32)
    for s in (4, 3, 5, 2, 6, 1, 7):
        last = last + shift(chunk_for((z + s) % NZ), "z", s).astype(F32)
    proj = jnp.concatenate([last[:chunk], done[:chunk]], axis=1).astype(BF)
    proj = lax.ppermute(proj, ("x", "z", "c", "y"), final_places()).astype(F32)
    head_sum = jnp.concatenate([last[chunk:], head_0], axis=1)
    both = other_core(head_sum)
    whole_sum = jnp.concatenate(
        [jnp.where(first, head_sum, both), jnp.where(first, both, head_sum)], axis=1
    ).T
    head_grad = gain.astype(F32)[:, None] * whole_sum
    gain_grad = jnp.sum(heads.astype(F32) * whole_sum, axis=1)

    reward_sums = reward_sums / (resp * NX * NZ)
    center, second = reward_sums[:, 0], reward_sums[:, 1]
    spread = second - center * center
    zed = (rewards[:, :resp_own] - center[:, None]) * lax.rsqrt(spread + EPS_VAR)[:, None]
    zmean = jnp.mean(zed, axis=0)
    uwo = zmean - PENALTY * jnp.mean((zed - zmean[None]) ** 2, axis=0)
    return (uwo, proj, head_grad, gain_grad)


def solution(mesh):
    finer = Mesh(mesh.devices.reshape(NX, NZ, NC, NY), ("x", "z", "c", "y"))
    dp = ("x", "z", "c")
    in_specs = (P(dp, "y"), P(dp, "y"), P("y", None), P("y", None), P("y"), P(dp))
    out_specs = (P(dp), P(dp, "y"), P("y", None), P("y"))
    return jax.shard_map(step, mesh=finer, in_specs=in_specs, out_specs=out_specs, check_vma=False)
```

```python
import jax
import jax.numpy as jnp
from jax import lax
from jax.experimental import pallas as pl
from jax.experimental.pallas import tpu as pltpu
from jax.sharding import Mesh
from jax.sharding import PartitionSpec as P

D = 5120
SEQ = 64
EPS_NORM = 1e-06
EPS_VAR = 1e-05
PENALTY = 0.5
NX, NZ, NC, NY = 4, 8, 2, 4
LANES = 128
CUT = 384
ROWS = 256
MIB = 2**20
HI = lax.Precision.HIGHEST
BF = jnp.bfloat16
F32 = jnp.float32


together = lax.optimization_barrier


def exchanged(x, axis):
    return lax.all_to_all(x, axis, split_axis=0, concat_axis=0, tiled=True)


def shift(x, axis, by):
    n = lax.axis_size(axis)
    return lax.ppermute(x, axis, [(i, (i + by) % n) for i in range(n)])


def other_core(x):
    return lax.ppermute(x, "c", [(0, 1), (1, 0)])


def shift_by_core(x, axis):
    n = lax.axis_size(axis)
    moves = [(c, i, (i + 1 - 2 * c) % n) for c in range(NC) for i in range(n)]
    if axis == "y":
        return lax.ppermute(x, ("c", axis), [(c * n + i, c * n + j) for c, i, j in moves])
    return lax.ppermute(x, (axis, "c"), [(i * NC + c, j * NC + c) for c, i, j in moves])


def chunk_of(z, c):
    if c == 0:
        return 2 * z if z < NZ // 2 else 2 * (NZ - 1 - z) + 1
    return 2 * (z - NZ // 2) + 1 if z >= NZ // 2 else 2 * (NZ // 2 - 1 - z)


def final_places():
    pairs = []
    for x in range(NX):
        for z in range(NZ):
            for c in range(NC):
                for y in range(NY):
                    src = ((x * NZ + z) * NC + c) * NY + y
                    q = chunk_of(z, c)
                    dst = ((y * NZ + 4 * c + q // 2) * NC + q % 2) * NY + (y + x) % NY
                    pairs.append((src, dst))
    return pairs


def in_pieces(v, count):
    pieces = []
    for _ in range(count):
        high = lax.reduce_precision(v, 8, 7)
        pieces.append(high.astype(BF))
        v = v - high
    return pieces


def line_rows(line, count):
    return jnp.concatenate(in_pieces(line, count), axis=0)


def rows_line(rows, members):
    rows = rows.astype(F32)
    return sum(rows[i : i + members] for i in range(0, rows.shape[0], members))


def sum_rows(sums):
    small = jnp.concatenate(in_pieces(sums, 3), axis=1)
    return jnp.pad(small, ((0, 0), (0, LANES - small.shape[1])))


def rows_sum(rows):
    small = rows[:, :6].astype(F32)
    return small[:, 0:2] + small[:, 2:4] + small[:, 4:6]


def gathered_weight(out_proj, x, y, c):
    block = out_proj.shape[0]
    half = out_proj.shape[1] // (NY * NC)
    rows = block // NX
    picked = lax.dynamic_slice_in_dim(out_proj, x * rows, rows, 0)
    sent = jnp.stack(
        [lax.dynamic_slice_in_dim(picked, (2 * k + c) * half, half, 1) for k in range(NY)]
    )
    came = exchanged(sent, "y")
    own = jnp.stack(
        [lax.dynamic_index_in_dim(came, (y + r) % NY, 0, keepdims=False) for r in (1, 2, 3)]
    )
    low, high = shift(own, "x", 1), shift(own, "x", -1)
    low, high, onward = together((low, high, jnp.where(c == 0, low, high)))
    far = shift_by_core(onward, "x")
    return sent, (own, low, high, far)


def split(v):
    high = v.astype(BF)
    return high, (v - high.astype(F32)).astype(BF)


def dot(a, b):
    return jnp.dot(a, b, preferred_element_type=F32)


def hidden_kernel(where, *refs):
    rows, refs = refs[: NC * NY], refs[NC * NY :]
    out_proj, w_own, w_low, w_high, w_far, resid, pack, gh, hidden, sums, *refs = refs
    turned, a, w, res, sem = refs
    y, c, x = where[0], where[1], where[2]
    count, half = rows[0].shape
    part = w_own.shape[1]
    halves = (slice(0, count), slice(count, 2 * count))
    columns = lambda i: pl.ds(pl.multiple_of(i * half, LANES), half)
    copies = []

    def fetch(src, dst):
        copies.append(pltpu.make_async_copy(src, dst, sem.at[len(copies)]))
        copies[-1].start()
        return copies[-1]

    ready = [fetch(out_proj.at[:, columns(2 * y + c)], w.at[0])]
    for piece, owner in ((w_own, x), (w_low, x + NX - 1), (w_high, x + 1), (w_far, x + 2)):
        at = pl.ds(pl.multiple_of(lax.rem(owner, NX) * part, part), part)
        ready.append(fetch(piece, w.at[1:NY, at, :]))
    for i, r in enumerate((resid.at[:, columns(c)], pack.at[halves[0], :])):
        ready.append(fetch(r, res.at[halves[i], :]))
        for k in range(NY):
            ready.append(fetch(rows[NC * k + i], a.at[halves[i], k * half : (k + 1) * half]))
    early = len(ready) - NY - 1
    blocks = count // ROWS
    g_high, g_low = split(gh[...])
    lane = lax.broadcasted_iota(jnp.int32, (ROWS, LANES), 1)
    members = sums.shape[0] // 2

    def multiply(base):
        @pl.loop(0, blocks)
        def _(i):
            here = pl.ds(pl.multiple_of(base + i * ROWS, ROWS), ROWS)
            acc = res[here, :].astype(F32) + dot(a[here, :], w[...].reshape(NY * half, half))
            hidden[here, :] = acc
            high, low = split(acc)
            tile = dot(high, g_high) + dot(high, g_low) + dot(low, g_high)
            squares = jnp.sum(acc * acc, axis=1, keepdims=True)
            tile = jnp.where(lane == members, squares, tile).T
            sums[:, here] = tile[: 2 * members]

    for copy in ready[:early]:
        copy.wait()
    multiply(0)
    for copy in ready[early:]:
        copy.wait()
    whole = NC * count
    moved = [
        fetch(a.at[:, columns(lax.rem(x + s, NX))], turned.at[s * whole : (s + 1) * whole])
        for s in range(NX)
    ]
    multiply(count)
    for copy in moved:
        copy.wait()


def hidden_and_sums(where, rows, out_proj, weights, resid, pack, gh):
    count, half = rows[0].shape
    members = gh.shape[1]
    total = NC * count
    gh = jnp.pad(gh, ((0, 0), (0, LANES - members)))
    any_space = pl.BlockSpec(memory_space=pl.ANY)
    full = lambda shape: pl.BlockSpec(shape, lambda i, s: (0, 0))
    return pl.pallas_call(
        hidden_kernel,
        grid_spec=pltpu.PrefetchScalarGridSpec(
            num_scalar_prefetch=1,
            grid=(1,),
            in_specs=[any_space] * (NC * NY + 7) + [full(gh.shape)],
            out_specs=[full((total, half)), full((2 * members, total)), any_space],
            scratch_shapes=[
                pltpu.VMEM((total, NY * half), BF),
                pltpu.VMEM((NY, half, half), BF),
                pltpu.VMEM((total, half), BF),
                pltpu.SemaphoreType.DMA((24,)),
            ],
        ),
        out_shape=[
            jax.ShapeDtypeStruct((total, half), F32),
            jax.ShapeDtypeStruct((2 * members, total), F32),
            jax.ShapeDtypeStruct((NX * total, half), BF),
        ],
        compiler_params=pltpu.CompilerParams(vmem_limit_bytes=52 * MIB),
        cost_estimate=pl.CostEstimate(
            flops=8 * total * half * half, bytes_accessed=20 * MIB, transcendentals=0
        ),
        name="hidden_and_sums",
    )(where, *rows, out_proj, *weights, resid, pack, gh)


def step(attn_out, resid, out_proj, heads, gain, lengths):
    x, c, y = (lax.axis_index(a) for a in ("x", "c", "y"))
    count, block = attn_out.shape
    members = heads.shape[1]
    half = resid.shape[1] // NC
    resp_own = lengths.shape[0]
    first = c == 0

    def own_half(a, axis, which):
        return lax.dynamic_slice_in_dim(a, which * half, half, axis)

    sent, weights = gathered_weight(out_proj, x, y, c)
    attn = together((attn_out, sent))[0]
    before, after = shift(attn, "y", 1), shift(attn, "y", -1)
    far = shift_by_core(jnp.where(first, before, after), "y")
    rows = [b for a in (attn, after, far, before) for b in (a, other_core(a))]
    lens_rows = jnp.zeros((8, half), BF).at[0, :resp_own].set(lengths.astype(BF))
    pack = jnp.concatenate([own_half(resid, 1, 1 - c), lens_rows], axis=0)
    pack = other_core(pack)
    lens = jnp.concatenate([lengths, pack[count, :resp_own].astype(jnp.int32)])
    total_rows, resp = 2 * count, 2 * resp_own
    gain_heads = own_half(gain, 0, c).astype(F32)[:, None] * own_half(heads, 0, c).astype(F32)
    where = jnp.stack([y, c, x]).astype(jnp.int32)
    hidden, part, turned = hidden_and_sums(
        where, rows, out_proj, weights, resid, pack, gain_heads
    )
    other = other_core(part)
    part = part + jnp.concatenate([other[:, count:], other[:, :count]], axis=1)
    part = part + shift(part, "y", 1) + shift(part, "y", -1) + shift(part, "y", 2)
    raw, squares = part[:members], part[members]

    rinv = lax.rsqrt(squares / D + EPS_NORM)
    scores = raw * rinv[None]
    counts = (lens + 1).astype(F32)
    at = lax.broadcasted_iota(jnp.int32, (resp, total_rows), 1) - SEQ * lax.broadcasted_iota(
        jnp.int32, (resp, total_rows), 0
    )
    inside = ((at >= 0) & (at <= lens[:, None])).astype(F32)
    rewards = jnp.einsum("kr,nr->kn", scores, inside, precision=HI) / counts[None]
    odd = lax.broadcasted_iota(jnp.int32, rewards.shape, 1) % 2 == 1
    partner = jnp.where(odd, jnp.roll(rewards, 1, 1), jnp.roll(rewards, -1, 1))
    sign = jnp.where(odd, 1.0, -1.0)
    dreward = sign * jax.nn.sigmoid(sign * (rewards - partner))
    dscore = jnp.einsum("kn,nr->kr", dreward / counts[None], inside, precision=HI)
    scaled = dscore * rinv[None]
    pull = rinv**3 * jnp.sum(dscore * raw, axis=0) / D
    s_high, s_low = in_pieces(scaled, 2)
    g_high, g_low = in_pieces(together((gain_heads.T, hidden))[0], 2)
    left = jnp.concatenate([s_high, s_low, s_high], axis=0)
    right = jnp.concatenate([g_high, g_high, g_low], axis=0)
    dhidden = (
        jnp.einsum("kr,kd->rd", left, right, preferred_element_type=F32) - hidden * pull[:, None]
    ).astype(BF)
    line = jnp.einsum("kr,rd->kd", scaled, hidden)
    sums = jnp.stack([jnp.sum(rewards, axis=1), jnp.sum(rewards * rewards, axis=1)], axis=1)

    near_a, up_a, far_a, down_a = (
        turned[i * total_rows : (i + 1) * total_rows] for i in range(NX)
    )
    far_a = together(far_a)

    def term(left, right):
        return jnp.einsum("rd,rj->dj", left, right, preferred_element_type=F32)

    slabs = (slice(CUT, None), slice(0, CUT))
    tiles = -(-block // CUT)
    line = jnp.pad(line, ((0, 0), (0, tiles * CUT - block)))
    line = jnp.concatenate([line[:, i * CUT : (i + 1) * CUT] for i in range(tiles)], axis=0)
    tall = line.shape[0]
    lines, extras = [None, line], [None, sums]

    def with_rows(body, head, extra, count):
        if head is None:
            return body
        small = jnp.pad(sum_rows(extra), ((0, 0), (0, CUT - LANES)))
        return jnp.concatenate([body, line_rows(head, count), small], axis=0)

    def read_rows(rows, head):
        if head is None:
            return None, None
        return rows_line(rows[:-members], tall), rows_sum(rows[-members:])

    came = []
    for lanes, head, extra in zip(slabs, lines, extras):
        outward = with_rows(term(dhidden, far_a[:, lanes]).astype(BF), head, extra, 2)
        outward, dhidden = together((outward, dhidden))
        came.append(shift_by_core(outward, "x"))
    up, down = together(tuple(term(dhidden, t) for t in (up_a, down_a)))
    near = together(term(dhidden, near_a))

    sends = []
    for lanes, head, extra, got in zip(slabs, lines, extras, came):
        arrived = got[:half].astype(F32)
        got_head, got_extra = read_rows(got[half:], head)

        def passed_on(t, use):
            body = (t[:, lanes] + jnp.where(use, arrived, 0.0)).astype(BF)
            if head is None:
                return body
            more = extra + jnp.where(use, got_extra, 0.0)
            return with_rows(body, head + jnp.where(use, got_head, 0.0), more, 2)

        pair = together((passed_on(up, first), passed_on(down, ~first)))
        got_up = shift(pair[0], "x", 1)
        got_down = shift(pair[1], "x", -1)
        sends.append((got_up, got_down))

    chunk = half // NZ
    totals = []
    for lanes, head, extra, (got_up, got_down) in zip(slabs, lines, extras, sends):
        body = near[:, lanes] + got_up[:half].astype(F32) + got_down[:half].astype(F32)
        if head is not None:
            up_head, up_extra = read_rows(got_up[half:], head)
            down_head, down_extra = read_rows(got_down[half:], head)
            head, extra = head + up_head + down_head, extra + up_extra + down_extra
        totals.append(together((body.astype(BF), head, extra)))

    body = totals[0][0].reshape(NZ, chunk, -1)
    orders = [jnp.stack([body[chunk_of(k, core)] for k in range(NZ)]) for core in range(NC)]
    done = exchanged(jnp.where(first, *orders), "z")
    done = done.astype(F32).sum(axis=0)

    body, head, extra = totals[1]
    rows = with_rows(body[:0], head, extra, 1)

    def chunk_for(to):
        low = jnp.where(first, 2 * to, 2 * (NZ // 2 - 1 - to))
        high = jnp.where(first, 2 * (NZ - 1 - to) + 1, 2 * (to - NZ // 2) + 1)
        at = jnp.where(to < NZ // 2, low, high) * chunk
        return jnp.concatenate([lax.dynamic_slice_in_dim(body, at, chunk, 0), rows], axis=0)

    z = lax.axis_index("z")
    last = chunk_for(z).astype(F32)
    for s in (4, 3, 5, 2, 6, 1, 7):
        last = last + shift(chunk_for((z + s) % NZ), "z", s).astype(F32)
    proj = jnp.concatenate([last[:chunk], done], axis=1).astype(BF)
    proj = lax.ppermute(proj, ("x", "z", "c", "y"), final_places()).astype(F32)
    head_sum = last[chunk : chunk + tall]
    head_sum = jnp.concatenate([head_sum[i : i + members] for i in range(0, tall, members)], axis=1)
    head_sum, reward_sums = head_sum[:, :block], rows_sum(last[-members:])
    both = other_core(head_sum)
    whole_sum = jnp.concatenate(
        [jnp.where(first, head_sum, both), jnp.where(first, both, head_sum)], axis=1
    ).T
    head_grad = gain.astype(F32)[:, None] * whole_sum
    gain_grad = jnp.sum(heads.astype(F32) * whole_sum, axis=1)

    reward_sums = reward_sums / (resp * NX * NZ)
    center, second = reward_sums[:, 0], reward_sums[:, 1]
    spread = second - center * center
    zed = (rewards[:, :resp_own] - center[:, None]) * lax.rsqrt(spread + EPS_VAR)[:, None]
    zmean = jnp.mean(zed, axis=0)
    uwo = zmean - PENALTY * jnp.mean((zed - zmean[None]) ** 2, axis=0)
    return (uwo, proj, head_grad, gain_grad)


def solution(mesh):
    finer = Mesh(mesh.devices.reshape(NX, NZ, NC, NY), ("x", "z", "c", "y"))
    dp = ("x", "z", "c")
    in_specs = (P(dp, "y"), P(dp, "y"), P("y", None), P("y", None), P("y"), P(dp))
    out_specs = (P(dp), P(dp, "y"), P("y", None), P("y"))
    return jax.shard_map(step, mesh=finer, in_specs=in_specs, out_specs=out_specs, check_vma=False)
```

```python
import jax
import jax.numpy as jnp
from jax import lax
from jax.experimental import pallas as pl
from jax.experimental.pallas import tpu as pltpu
from jax.sharding import Mesh
from jax.sharding import PartitionSpec as P

D = 5120
SEQ = 64
EPS_NORM = 1e-06
EPS_VAR = 1e-05
PENALTY = 0.5
NX, NZ, NC, NY = 4, 8, 2, 4
LANES = 128
CUT = 384
ROWS = 256
MIB = 2**20
HI = lax.Precision.HIGHEST
BF = jnp.bfloat16
F32 = jnp.float32


together = lax.optimization_barrier


def exchanged(x, axis):
    return lax.all_to_all(x, axis, split_axis=0, concat_axis=0, tiled=True)


def shift(x, axis, by):
    n = lax.axis_size(axis)
    return lax.ppermute(x, axis, [(i, (i + by) % n) for i in range(n)])


def other_core(x):
    return lax.ppermute(x, "c", [(0, 1), (1, 0)])


def shift_by_core(x, axis):
    n = lax.axis_size(axis)
    moves = [(c, i, (i + 1 - 2 * c) % n) for c in range(NC) for i in range(n)]
    if axis == "y":
        return lax.ppermute(x, ("c", axis), [(c * n + i, c * n + j) for c, i, j in moves])
    return lax.ppermute(x, (axis, "c"), [(i * NC + c, j * NC + c) for c, i, j in moves])


def chunk_of(z, c):
    if c == 0:
        return 2 * z if z < NZ // 2 else 2 * (NZ - 1 - z) + 1
    return 2 * (z - NZ // 2) + 1 if z >= NZ // 2 else 2 * (NZ // 2 - 1 - z)


def final_places():
    pairs = []
    for x in range(NX):
        for z in range(NZ):
            for c in range(NC):
                for y in range(NY):
                    src = ((x * NZ + z) * NC + c) * NY + y
                    q = chunk_of(z, c)
                    dst = ((y * NZ + 4 * c + q // 2) * NC + q % 2) * NY + (y + x) % NY
                    pairs.append((src, dst))
    return pairs


def in_pieces(v, count):
    pieces = []
    for _ in range(count):
        high = lax.reduce_precision(v, 8, 7)
        pieces.append(high.astype(BF))
        v = v - high
    return pieces


def line_rows(line, count):
    return jnp.concatenate(in_pieces(line, count), axis=0)


def rows_line(rows, members):
    rows = rows.astype(F32)
    return sum(rows[i : i + members] for i in range(0, rows.shape[0], members))


def sum_rows(sums):
    small = jnp.concatenate(in_pieces(sums, 3), axis=1)
    return jnp.pad(small, ((0, 0), (0, LANES - small.shape[1])))


def rows_sum(rows):
    small = rows[:, :6].astype(F32)
    return small[:, 0:2] + small[:, 2:4] + small[:, 4:6]


def gathered_weight(out_proj, x, y, c):
    block = out_proj.shape[0]
    half = out_proj.shape[1] // (NY * NC)
    rows = block // NX
    picked = lax.dynamic_slice_in_dim(out_proj, x * rows, rows, 0)
    sent = jnp.stack(
        [lax.dynamic_slice_in_dim(picked, (2 * k + c) * half, half, 1) for k in range(NY)]
    )
    came = exchanged(sent, "y")
    own = jnp.stack(
        [lax.dynamic_index_in_dim(came, (y + r) % NY, 0, keepdims=False) for r in (1, 2, 3)]
    )
    low, high = shift(own, "x", 1), shift(own, "x", -1)
    low, high, onward = together((low, high, jnp.where(c == 0, low, high)))
    far = shift_by_core(onward, "x")
    return sent, (own, low, high, far)


def split(v):
    high = v.astype(BF)
    return high, (v - high.astype(F32)).astype(BF)


def dot(a, b):
    return jnp.dot(a, b, preferred_element_type=F32)


def hidden_kernel(where, *refs):
    rows, refs = refs[: NC * NY], refs[NC * NY :]
    out_proj, w_own, w_low, w_high, w_far, resid, pack, gh, hidden_out, sums, *refs = refs
    turned, a, w, res, hidden, sem = refs
    y, c, x = where[0], where[1], where[2]
    count, half = rows[0].shape
    part = w_own.shape[1]
    halves = (slice(0, count), slice(count, 2 * count))
    columns = lambda i: pl.ds(pl.multiple_of(i * half, LANES), half)
    copies = []

    def fetch(src, dst):
        copies.append(pltpu.make_async_copy(src, dst, sem.at[len(copies)]))
        copies[-1].start()
        return copies[-1]

    ready = [fetch(out_proj.at[:, columns(2 * y + c)], w.at[0])]
    for piece, owner in ((w_own, x), (w_low, x + NX - 1), (w_high, x + 1), (w_far, x + 2)):
        at = pl.ds(pl.multiple_of(lax.rem(owner, NX) * part, part), part)
        ready.append(fetch(piece, w.at[1:NY, at, :]))
    for i, r in enumerate((resid.at[:, columns(c)], pack.at[halves[0], :])):
        ready.append(fetch(r, res.at[halves[i], :]))
        for k in range(NY):
            ready.append(fetch(rows[NC * k + i], a.at[halves[i], k * half : (k + 1) * half]))
    early = len(ready) - NY - 1
    blocks = count // ROWS
    g_high, g_low = split(gh[...])
    lane = lax.broadcasted_iota(jnp.int32, (ROWS, LANES), 1)
    members = sums.shape[0] // 2

    def multiply(base):
        @pl.loop(0, blocks)
        def _(i):
            here = pl.ds(pl.multiple_of(base + i * ROWS, ROWS), ROWS)
            acc = res[here, :].astype(F32) + dot(a[here, :], w[...].reshape(NY * half, half))
            hidden[here, :] = acc
            high, low = split(acc)
            tile = dot(high, g_high) + dot(high, g_low) + dot(low, g_high)
            squares = jnp.sum(acc * acc, axis=1, keepdims=True)
            tile = jnp.where(lane == members, squares, tile).T
            sums[:, here] = tile[: 2 * members]

    whole = NC * count

    def turn(rows):
        return [
            fetch(
                a.at[rows, columns(lax.rem(x + s, NX))],
                turned.at[s * whole + rows.start : s * whole + rows.stop],
            )
            for s in range(NX)
        ]

    for copy in ready[:early]:
        copy.wait()
    out = turn(halves[0])
    multiply(0)
    for copy in ready[early:]:
        copy.wait()
    out += turn(halves[1])
    out.append(fetch(hidden.at[halves[0]], hidden_out.at[halves[0]]))
    multiply(count)
    for copy in out:
        copy.wait()
    fetch(hidden.at[halves[1]], hidden_out.at[halves[1]]).wait()


def hidden_and_sums(where, rows, out_proj, weights, resid, pack, gh):
    count, half = rows[0].shape
    members = gh.shape[1]
    total = NC * count
    gh = jnp.pad(gh, ((0, 0), (0, LANES - members)))
    any_space = pl.BlockSpec(memory_space=pl.ANY)
    full = lambda shape: pl.BlockSpec(shape, lambda i, s: (0, 0))
    return pl.pallas_call(
        hidden_kernel,
        grid_spec=pltpu.PrefetchScalarGridSpec(
            num_scalar_prefetch=1,
            grid=(1,),
            in_specs=[any_space] * (NC * NY + 7) + [full(gh.shape)],
            out_specs=[any_space, full((2 * members, total)), any_space],
            scratch_shapes=[
                pltpu.VMEM((total, NY * half), BF),
                pltpu.VMEM((NY, half, half), BF),
                pltpu.VMEM((total, half), BF),
                pltpu.VMEM((total, half), F32),
                pltpu.SemaphoreType.DMA((25,)),
            ],
        ),
        out_shape=[
            jax.ShapeDtypeStruct((total, half), F32),
            jax.ShapeDtypeStruct((2 * members, total), F32),
            jax.ShapeDtypeStruct((NX * total, half), BF),
        ],
        compiler_params=pltpu.CompilerParams(vmem_limit_bytes=52 * MIB),
        cost_estimate=pl.CostEstimate(
            flops=8 * total * half * half, bytes_accessed=20 * MIB, transcendentals=0
        ),
        name="hidden_and_sums",
    )(where, *rows, out_proj, *weights, resid, pack, gh)


def step(attn_out, resid, out_proj, heads, gain, lengths):
    x, c, y = (lax.axis_index(a) for a in ("x", "c", "y"))
    count, block = attn_out.shape
    members = heads.shape[1]
    half = resid.shape[1] // NC
    resp_own = lengths.shape[0]
    first = c == 0

    def own_half(a, axis, which):
        return lax.dynamic_slice_in_dim(a, which * half, half, axis)

    sent, weights = gathered_weight(out_proj, x, y, c)
    attn = together((attn_out, sent))[0]
    before, after = shift(attn, "y", 1), shift(attn, "y", -1)
    far = shift_by_core(jnp.where(first, before, after), "y")
    rows = [b for a in (attn, after, far, before) for b in (a, other_core(a))]
    lens_rows = jnp.zeros((8, half), BF).at[0, :resp_own].set(lengths.astype(BF))
    pack = jnp.concatenate([own_half(resid, 1, 1 - c), lens_rows], axis=0)
    pack = other_core(pack)
    lens = jnp.concatenate([lengths, pack[count, :resp_own].astype(jnp.int32)])
    total_rows, resp = 2 * count, 2 * resp_own
    gain_heads = own_half(gain, 0, c).astype(F32)[:, None] * own_half(heads, 0, c).astype(F32)
    where = jnp.stack([y, c, x]).astype(jnp.int32)
    hidden, part, turned = hidden_and_sums(
        where, rows, out_proj, weights, resid, pack, gain_heads
    )
    other = other_core(part)
    part = part + jnp.concatenate([other[:, count:], other[:, :count]], axis=1)
    part = part + shift(part, "y", 1) + shift(part, "y", -1) + shift(part, "y", 2)
    raw, squares = part[:members], part[members]

    rinv = lax.rsqrt(squares / D + EPS_NORM)
    scores = raw * rinv[None]
    counts = (lens + 1).astype(F32)
    at = lax.broadcasted_iota(jnp.int32, (resp, total_rows), 1) - SEQ * lax.broadcasted_iota(
        jnp.int32, (resp, total_rows), 0
    )
    inside = ((at >= 0) & (at <= lens[:, None])).astype(F32)
    rewards = jnp.einsum("kr,nr->kn", scores, inside, precision=HI) / counts[None]
    odd = lax.broadcasted_iota(jnp.int32, rewards.shape, 1) % 2 == 1
    partner = jnp.where(odd, jnp.roll(rewards, 1, 1), jnp.roll(rewards, -1, 1))
    sign = jnp.where(odd, 1.0, -1.0)
    dreward = sign * jax.nn.sigmoid(sign * (rewards - partner))
    dscore = jnp.einsum("kn,nr->kr", dreward / counts[None], inside, precision=HI)
    scaled = dscore * rinv[None]
    pull = rinv**3 * jnp.sum(dscore * raw, axis=0) / D
    s_high, s_low = in_pieces(scaled, 2)
    g_high, g_low = in_pieces(together((gain_heads.T, hidden))[0], 2)
    left = jnp.concatenate([s_high, s_low, s_high], axis=0)
    right = jnp.concatenate([g_high, g_high, g_low], axis=0)
    dhidden = (
        jnp.einsum("kr,kd->rd", left, right, preferred_element_type=F32) - hidden * pull[:, None]
    ).astype(BF)
    line = jnp.einsum("kr,rd->kd", scaled, hidden)
    sums = jnp.stack([jnp.sum(rewards, axis=1), jnp.sum(rewards * rewards, axis=1)], axis=1)

    near_a, up_a, far_a, down_a = (
        turned[i * total_rows : (i + 1) * total_rows] for i in range(NX)
    )
    far_a = together(far_a)

    def term(left, right):
        return jnp.einsum("rd,rj->dj", left, right, preferred_element_type=F32)

    slabs = (slice(CUT, None), slice(0, CUT))
    tiles = -(-block // CUT)
    line = jnp.pad(line, ((0, 0), (0, tiles * CUT - block)))
    line = jnp.concatenate([line[:, i * CUT : (i + 1) * CUT] for i in range(tiles)], axis=0)
    tall = line.shape[0]
    lines, extras = [None, line], [None, sums]

    def with_rows(body, head, extra, count):
        if head is None:
            return body
        small = jnp.pad(sum_rows(extra), ((0, 0), (0, CUT - LANES)))
        return jnp.concatenate([body, line_rows(head, count), small], axis=0)

    def read_rows(rows, head):
        if head is None:
            return None, None
        return rows_line(rows[:-members], tall), rows_sum(rows[-members:])

    came = []
    for lanes, head, extra in zip(slabs, lines, extras):
        outward = with_rows(term(dhidden, far_a[:, lanes]).astype(BF), head, extra, 2)
        outward, dhidden = together((outward, dhidden))
        came.append(shift_by_core(outward, "x"))
    up, down = together(tuple(term(dhidden, t) for t in (up_a, down_a)))
    near = together(term(dhidden, near_a))

    sends = []
    for lanes, head, extra, got in zip(slabs, lines, extras, came):
        arrived = got[:half].astype(F32)
        got_head, got_extra = read_rows(got[half:], head)

        def passed_on(t, use):
            body = (t[:, lanes] + jnp.where(use, arrived, 0.0)).astype(BF)
            if head is None:
                return body
            more = extra + jnp.where(use, got_extra, 0.0)
            return with_rows(body, head + jnp.where(use, got_head, 0.0), more, 2)

        pair = together((passed_on(up, first), passed_on(down, ~first)))
        got_up = shift(pair[0], "x", 1)
        got_down = shift(pair[1], "x", -1)
        sends.append((got_up, got_down))

    chunk = half // NZ
    totals = []
    for lanes, head, extra, (got_up, got_down) in zip(slabs, lines, extras, sends):
        body = near[:, lanes] + got_up[:half].astype(F32) + got_down[:half].astype(F32)
        if head is not None:
            up_head, up_extra = read_rows(got_up[half:], head)
            down_head, down_extra = read_rows(got_down[half:], head)
            head, extra = head + up_head + down_head, extra + up_extra + down_extra
        totals.append(together((body.astype(BF), head, extra)))

    body = totals[0][0].reshape(NZ, chunk, -1)
    orders = [jnp.stack([body[chunk_of(k, core)] for k in range(NZ)]) for core in range(NC)]
    done = exchanged(jnp.where(first, *orders), "z")
    done = done.astype(F32).sum(axis=0)

    body, head, extra = totals[1]
    rows = with_rows(body[:0], head, extra, 1)

    def chunk_for(to):
        low = jnp.where(first, 2 * to, 2 * (NZ // 2 - 1 - to))
        high = jnp.where(first, 2 * (NZ - 1 - to) + 1, 2 * (to - NZ // 2) + 1)
        at = jnp.where(to < NZ // 2, low, high) * chunk
        return jnp.concatenate([lax.dynamic_slice_in_dim(body, at, chunk, 0), rows], axis=0)

    z = lax.axis_index("z")
    last = chunk_for(z).astype(F32)
    for s in (4, 3, 5, 2, 6, 1, 7):
        last = last + shift(chunk_for((z + s) % NZ), "z", s).astype(F32)
    proj = jnp.concatenate([last[:chunk], done], axis=1).astype(BF)
    proj = lax.ppermute(proj, ("x", "z", "c", "y"), final_places()).astype(F32)
    head_sum = last[chunk : chunk + tall]
    head_sum = jnp.concatenate([head_sum[i : i + members] for i in range(0, tall, members)], axis=1)
    head_sum, reward_sums = head_sum[:, :block], rows_sum(last[-members:])
    both = other_core(head_sum)
    whole_sum = jnp.concatenate(
        [jnp.where(first, head_sum, both), jnp.where(first, both, head_sum)], axis=1
    ).T
    head_grad = gain.astype(F32)[:, None] * whole_sum
    gain_grad = jnp.sum(heads.astype(F32) * whole_sum, axis=1)

    reward_sums = reward_sums / (resp * NX * NZ)
    center, second = reward_sums[:, 0], reward_sums[:, 1]
    spread = second - center * center
    zed = (rewards[:, :resp_own] - center[:, None]) * lax.rsqrt(spread + EPS_VAR)[:, None]
    zmean = jnp.mean(zed, axis=0)
    uwo = zmean - PENALTY * jnp.mean((zed - zmean[None]) ** 2, axis=0)
    return (uwo, proj, head_grad, gain_grad)


def solution(mesh):
    finer = Mesh(mesh.devices.reshape(NX, NZ, NC, NY), ("x", "z", "c", "y"))
    dp = ("x", "z", "c")
    in_specs = (P(dp, "y"), P(dp, "y"), P("y", None), P("y", None), P("y"), P(dp))
    out_specs = (P(dp), P(dp, "y"), P("y", None), P("y"))
    return jax.shard_map(step, mesh=finer, in_specs=in_specs, out_specs=out_specs, check_vma=False)
```

```python
import jax
import jax.numpy as jnp
from jax import lax
from jax.experimental import pallas as pl
from jax.experimental.pallas import tpu as pltpu
from jax.sharding import Mesh
from jax.sharding import PartitionSpec as P

D = 5120
SEQ = 64
EPS_NORM = 1e-06
EPS_VAR = 1e-05
PENALTY = 0.5
NX, NZ, NC, NY = 4, 8, 2, 4
LANES = 128
CUT = 384
ROWS = 256
MIB = 2**20
HI = lax.Precision.HIGHEST
BF = jnp.bfloat16
F32 = jnp.float32


together = lax.optimization_barrier


def exchanged(x, axis):
    return lax.all_to_all(x, axis, split_axis=0, concat_axis=0, tiled=True)


def shift(x, axis, by):
    n = lax.axis_size(axis)
    return lax.ppermute(x, axis, [(i, (i + by) % n) for i in range(n)])


def other_core(x):
    return lax.ppermute(x, "c", [(0, 1), (1, 0)])


def shift_by_core(x, axis):
    n = lax.axis_size(axis)
    moves = [(c, i, (i + 1 - 2 * c) % n) for c in range(NC) for i in range(n)]
    if axis == "y":
        return lax.ppermute(x, ("c", axis), [(c * n + i, c * n + j) for c, i, j in moves])
    return lax.ppermute(x, (axis, "c"), [(i * NC + c, j * NC + c) for c, i, j in moves])


def chunk_of(z, c):
    if c == 0:
        return 2 * z if z < NZ // 2 else 2 * (NZ - 1 - z) + 1
    return 2 * (z - NZ // 2) + 1 if z >= NZ // 2 else 2 * (NZ // 2 - 1 - z)


def final_places():
    pairs = []
    for x in range(NX):
        for z in range(NZ):
            for c in range(NC):
                for y in range(NY):
                    src = ((x * NZ + z) * NC + c) * NY + y
                    q = chunk_of(z, c)
                    dst = ((y * NZ + 4 * c + q // 2) * NC + q % 2) * NY + (y + x) % NY
                    pairs.append((src, dst))
    return pairs


def in_pieces(v, count):
    pieces = []
    for _ in range(count):
        high = lax.reduce_precision(v, 8, 7)
        pieces.append(high.astype(BF))
        v = v - high
    return pieces


def line_rows(line, count):
    return jnp.concatenate(in_pieces(line, count), axis=0)


def rows_line(rows, members):
    rows = rows.astype(F32)
    return sum(rows[i : i + members] for i in range(0, rows.shape[0], members))


def sum_rows(sums):
    small = jnp.concatenate(in_pieces(sums, 3), axis=1)
    return jnp.pad(small, ((0, 0), (0, LANES - small.shape[1])))


def rows_sum(rows):
    small = rows[:, :6].astype(F32)
    return small[:, 0:2] + small[:, 2:4] + small[:, 4:6]


def gathered_weight(out_proj, x, y, c):
    block = out_proj.shape[0]
    half = out_proj.shape[1] // (NY * NC)
    rows = block // NX
    picked = lax.dynamic_slice_in_dim(out_proj, x * rows, rows, 0)
    sent = jnp.stack(
        [lax.dynamic_slice_in_dim(picked, (2 * k + c) * half, half, 1) for k in range(NY)]
    )
    came = exchanged(sent, "y")
    own = jnp.stack(
        [lax.dynamic_index_in_dim(came, (y + r) % NY, 0, keepdims=False) for r in (1, 2, 3)]
    )
    low, high = shift(own, "x", 1), shift(own, "x", -1)
    low, high, onward = together((low, high, jnp.where(c == 0, low, high)))
    far = shift_by_core(onward, "x")
    return sent, (own, low, high, far)


def split(v):
    high = v.astype(BF)
    return high, (v - high.astype(F32)).astype(BF)


def dot(a, b):
    return jnp.dot(a, b, preferred_element_type=F32)


def hidden_kernel(where, *refs):
    rows, refs = refs[: NC * NY], refs[NC * NY :]
    out_proj, w_own, w_low, w_high, w_far, resid, pack, gh, hidden, sums, *refs = refs
    turned, a, w, res, sem = refs
    y, c, x = where[0], where[1], where[2]
    count, half = rows[0].shape
    part = w_own.shape[1]
    halves = (slice(0, count), slice(count, 2 * count))
    columns = lambda i: pl.ds(pl.multiple_of(i * half, LANES), half)
    copies = []

    def fetch(src, dst):
        copies.append(pltpu.make_async_copy(src, dst, sem.at[len(copies)]))
        copies[-1].start()
        return copies[-1]

    ready = [fetch(out_proj.at[:, columns(2 * y + c)], w.at[0])]
    for piece, owner in ((w_own, x), (w_low, x + NX - 1), (w_high, x + 1), (w_far, x + 2)):
        at = pl.ds(pl.multiple_of(lax.rem(owner, NX) * part, part), part)
        ready.append(fetch(piece, w.at[1:NY, at, :]))
    for i, r in enumerate((resid.at[:, columns(c)], pack.at[halves[0], :])):
        ready.append(fetch(r, res.at[halves[i], :]))
        for k in range(NY):
            ready.append(fetch(rows[NC * k + i], a.at[halves[i], k * half : (k + 1) * half]))
    early = len(ready) - NY - 1
    blocks = count // ROWS
    g_high, g_low = split(gh[...])
    lane = lax.broadcasted_iota(jnp.int32, (ROWS, LANES), 1)
    members = sums.shape[0] // 2

    def multiply(base):
        @pl.loop(0, blocks)
        def _(i):
            here = pl.ds(pl.multiple_of(base + i * ROWS, ROWS), ROWS)
            acc = res[here, :].astype(F32) + dot(a[here, :], w[...].reshape(NY * half, half))
            hidden[here, :] = acc
            high, low = split(acc)
            tile = dot(high, g_high) + dot(high, g_low) + dot(low, g_high)
            squares = jnp.sum(acc * acc, axis=1, keepdims=True)
            tile = jnp.where(lane == members, squares, tile).T
            sums[:, here] = tile[: 2 * members]

    whole = NC * count

    def turn(rows):
        return [
            fetch(
                a.at[rows, columns(lax.rem(x + s, NX))],
                turned.at[s * whole + rows.start : s * whole + rows.stop],
            )
            for s in range(NX)
        ]

    for copy in ready[:early]:
        copy.wait()
    out = turn(halves[0])
    multiply(0)
    for copy in ready[early:]:
        copy.wait()
    out += turn(halves[1])
    multiply(count)
    for copy in out:
        copy.wait()


def hidden_and_sums(where, rows, out_proj, weights, resid, pack, gh):
    count, half = rows[0].shape
    members = gh.shape[1]
    total = NC * count
    gh = jnp.pad(gh, ((0, 0), (0, LANES - members)))
    any_space = pl.BlockSpec(memory_space=pl.ANY)
    full = lambda shape: pl.BlockSpec(shape, lambda i, s: (0, 0))
    return pl.pallas_call(
        hidden_kernel,
        grid_spec=pltpu.PrefetchScalarGridSpec(
            num_scalar_prefetch=1,
            grid=(1,),
            in_specs=[any_space] * (NC * NY + 7) + [full(gh.shape)],
            out_specs=[full((total, half)), full((2 * members, total)), any_space],
            scratch_shapes=[
                pltpu.VMEM((total, NY * half), BF),
                pltpu.VMEM((NY, half, half), BF),
                pltpu.VMEM((total, half), BF),
                pltpu.SemaphoreType.DMA((23,)),
            ],
        ),
        out_shape=[
            jax.ShapeDtypeStruct((total, half), F32),
            jax.ShapeDtypeStruct((2 * members, total), F32),
            jax.ShapeDtypeStruct((NX * total, half), BF),
        ],
        compiler_params=pltpu.CompilerParams(vmem_limit_bytes=52 * MIB),
        cost_estimate=pl.CostEstimate(
            flops=8 * total * half * half, bytes_accessed=20 * MIB, transcendentals=0
        ),
        name="hidden_and_sums",
    )(where, *rows, out_proj, *weights, resid, pack, gh)


def step(attn_out, resid, out_proj, heads, gain, lengths):
    x, c, y = (lax.axis_index(a) for a in ("x", "c", "y"))
    count, block = attn_out.shape
    members = heads.shape[1]
    half = resid.shape[1] // NC
    resp_own = lengths.shape[0]
    first = c == 0

    def own_half(a, axis, which):
        return lax.dynamic_slice_in_dim(a, which * half, half, axis)

    sent, weights = gathered_weight(out_proj, x, y, c)
    attn = together((attn_out, sent))[0]
    before, after = shift(attn, "y", 1), shift(attn, "y", -1)
    far = shift_by_core(jnp.where(first, before, after), "y")
    rows = [b for a in (attn, after, far, before) for b in (a, other_core(a))]
    lens_rows = jnp.zeros((8, half), BF).at[0, :resp_own].set(lengths.astype(BF))
    pack = jnp.concatenate([own_half(resid, 1, 1 - c), lens_rows], axis=0)
    pack = other_core(pack)
    lens = jnp.concatenate([lengths, pack[count, :resp_own].astype(jnp.int32)])
    total_rows, resp = 2 * count, 2 * resp_own
    gain_heads = own_half(gain, 0, c).astype(F32)[:, None] * own_half(heads, 0, c).astype(F32)
    where = jnp.stack([y, c, x]).astype(jnp.int32)
    hidden, part, turned = hidden_and_sums(
        where, rows, out_proj, weights, resid, pack, gain_heads
    )
    other = other_core(part)
    part = part + jnp.concatenate([other[:, count:], other[:, :count]], axis=1)
    part = part + shift(part, "y", 1) + shift(part, "y", -1) + shift(part, "y", 2)
    raw, squares = part[:members], part[members]

    rinv = lax.rsqrt(squares / D + EPS_NORM)
    scores = raw * rinv[None]
    counts = (lens + 1).astype(F32)
    at = lax.broadcasted_iota(jnp.int32, (resp, total_rows), 1) - SEQ * lax.broadcasted_iota(
        jnp.int32, (resp, total_rows), 0
    )
    inside = ((at >= 0) & (at <= lens[:, None])).astype(F32)
    rewards = jnp.einsum("kr,nr->kn", scores, inside, precision=HI) / counts[None]
    odd = lax.broadcasted_iota(jnp.int32, rewards.shape, 1) % 2 == 1
    partner = jnp.where(odd, jnp.roll(rewards, 1, 1), jnp.roll(rewards, -1, 1))
    sign = jnp.where(odd, 1.0, -1.0)
    dreward = sign * jax.nn.sigmoid(sign * (rewards - partner))
    dscore = jnp.einsum("kn,nr->kr", dreward / counts[None], inside, precision=HI)
    scaled = dscore * rinv[None]
    pull = rinv**3 * jnp.sum(dscore * raw, axis=0) / D
    s_high, s_low = in_pieces(scaled, 2)
    g_high, g_low = in_pieces(together((gain_heads.T, hidden))[0], 2)
    left = jnp.concatenate([s_high, s_low, s_high], axis=0)
    right = jnp.concatenate([g_high, g_high, g_low], axis=0)
    dhidden = (
        jnp.einsum("kr,kd->rd", left, right, preferred_element_type=F32) - hidden * pull[:, None]
    ).astype(BF)
    line = jnp.einsum("kr,rd->kd", scaled, hidden)
    sums = jnp.stack([jnp.sum(rewards, axis=1), jnp.sum(rewards * rewards, axis=1)], axis=1)

    near_a, up_a, far_a, down_a = (
        turned[i * total_rows : (i + 1) * total_rows] for i in range(NX)
    )
    far_a = together(far_a)

    def term(left, right):
        return jnp.einsum("rd,rj->dj", left, right, preferred_element_type=F32)

    slabs = (slice(CUT, None), slice(0, CUT))
    tiles = -(-block // CUT)
    line = jnp.pad(line, ((0, 0), (0, tiles * CUT - block)))
    line = jnp.concatenate([line[:, i * CUT : (i + 1) * CUT] for i in range(tiles)], axis=0)
    tall = line.shape[0]
    lines, extras = [None, line], [None, sums]

    def with_rows(body, head, extra, count):
        if head is None:
            return body
        small = jnp.pad(sum_rows(extra), ((0, 0), (0, CUT - LANES)))
        return jnp.concatenate([body, line_rows(head, count), small], axis=0)

    def read_rows(rows, head):
        if head is None:
            return None, None
        return rows_line(rows[:-members], tall), rows_sum(rows[-members:])

    came = []
    for lanes, head, extra in zip(slabs, lines, extras):
        outward = with_rows(term(dhidden, far_a[:, lanes]).astype(BF), head, extra, 2)
        outward, dhidden = together((outward, dhidden))
        came.append(shift_by_core(outward, "x"))
    up, down = together(tuple(term(dhidden, t) for t in (up_a, down_a)))
    near = together(term(dhidden, near_a))

    sends = []
    for lanes, head, extra, got in zip(slabs, lines, extras, came):
        arrived = got[:half].astype(F32)
        got_head, got_extra = read_rows(got[half:], head)

        def passed_on(t, use):
            body = (t[:, lanes] + jnp.where(use, arrived, 0.0)).astype(BF)
            if head is None:
                return body
            more = extra + jnp.where(use, got_extra, 0.0)
            return with_rows(body, head + jnp.where(use, got_head, 0.0), more, 2)

        pair = together((passed_on(up, first), passed_on(down, ~first)))
        got_up = shift(pair[0], "x", 1)
        got_down = shift(pair[1], "x", -1)
        sends.append((got_up, got_down))

    chunk = half // NZ
    totals = []
    for lanes, head, extra, (got_up, got_down) in zip(slabs, lines, extras, sends):
        body = near[:, lanes] + got_up[:half].astype(F32) + got_down[:half].astype(F32)
        if head is not None:
            up_head, up_extra = read_rows(got_up[half:], head)
            down_head, down_extra = read_rows(got_down[half:], head)
            head, extra = head + up_head + down_head, extra + up_extra + down_extra
        totals.append(together((body.astype(BF), head, extra)))

    body = totals[0][0].reshape(NZ, chunk, -1)
    orders = [jnp.stack([body[chunk_of(k, core)] for k in range(NZ)]) for core in range(NC)]
    done = exchanged(jnp.where(first, *orders), "z")
    done = done.astype(F32).sum(axis=0)

    body, head, extra = totals[1]
    rows = with_rows(body[:0], head, extra, 1)

    def chunk_for(to):
        low = jnp.where(first, 2 * to, 2 * (NZ // 2 - 1 - to))
        high = jnp.where(first, 2 * (NZ - 1 - to) + 1, 2 * (to - NZ // 2) + 1)
        at = jnp.where(to < NZ // 2, low, high) * chunk
        return jnp.concatenate([lax.dynamic_slice_in_dim(body, at, chunk, 0), rows], axis=0)

    z = lax.axis_index("z")
    last = chunk_for(z).astype(F32)
    for s in (4, 3, 5, 2, 6, 1, 7):
        last = last + shift(chunk_for((z + s) % NZ), "z", s).astype(F32)
    proj = jnp.concatenate([last[:chunk], done], axis=1).astype(BF)
    proj = lax.ppermute(proj, ("x", "z", "c", "y"), final_places()).astype(F32)
    head_sum = last[chunk : chunk + tall]
    head_sum = jnp.concatenate([head_sum[i : i + members] for i in range(0, tall, members)], axis=1)
    head_sum, reward_sums = head_sum[:, :block], rows_sum(last[-members:])
    both = other_core(head_sum)
    whole_sum = jnp.concatenate(
        [jnp.where(first, head_sum, both), jnp.where(first, both, head_sum)], axis=1
    ).T
    head_grad = gain.astype(F32)[:, None] * whole_sum
    gain_grad = jnp.sum(heads.astype(F32) * whole_sum, axis=1)

    reward_sums = reward_sums / (resp * NX * NZ)
    center, second = reward_sums[:, 0], reward_sums[:, 1]
    spread = second - center * center
    zed = (rewards[:, :resp_own] - center[:, None]) * lax.rsqrt(spread + EPS_VAR)[:, None]
    zmean = jnp.mean(zed, axis=0)
    uwo = zmean - PENALTY * jnp.mean((zed - zmean[None]) ** 2, axis=0)
    return (uwo, proj, head_grad, gain_grad)


def solution(mesh):
    finer = Mesh(mesh.devices.reshape(NX, NZ, NC, NY), ("x", "z", "c", "y"))
    dp = ("x", "z", "c")
    in_specs = (P(dp, "y"), P(dp, "y"), P("y", None), P("y", None), P("y"), P(dp))
    out_specs = (P(dp), P(dp, "y"), P("y", None), P("y"))
    return jax.shard_map(step, mesh=finer, in_specs=in_specs, out_specs=out_specs, check_vma=False)
```
